32 devices in a mesh: gx: 4 (over z), gy: 2 (over y), gz: 4 (over x, core).
Axes of the slice: x: 2, y: 2, z: 4, core: 2. Of those that a mesh axis runs over, the one named last changes fastest.
Arguments:
- cell_volume: float32 [64, 32, 512], P('gx', 'gy', 'gz'), may hold values from 0.5 to 2
- exponent: int32 [64, 32, 512], P('gx', 'gy', 'gz'), may hold values from 0 to 7
- owner_row: int32 [8192], P(('gx', 'gy', 'gz')), may hold values from 0 to 8191, as said below
Outputs:
- stencil_out: float32 [27, 8192, 128], P(None, ('gx', 'gy', 'gz'))
- lumped_out: float32 [8192, 128], P(('gx', 'gy', 'gz'))
The draws below stay inside these ranges and needn't reach their ends.
Inputs may be any that keep to these rules, and one draw needn't show every extreme that they name: owner_row is a permutation of the row blocks; the row blocks of each device's share of owner_row go to each owner (owner_row // 256) exactly 8 times.
All inputs are finite; a program needn't handle non-finite values.
Results may differ from the reference program's by a relative error of at most 0.00007.
Values sent between devices are 32-bit elements; how exact they have to be, the bound alone decides.
A program may use at most 64 MiB of HBM per device.

```python
import math
import jax
import jax.numpy as jnp

EX = 16
EY = 16
EZ = 128
NX = 64
NY = 32
NZ = 512
LINES_DEV = 256
LINES = 8192
SENDS = 8
N_GX = 4
N_GY = 2
N_GZ = 4
DEVICES = 32


def draw_owner_row(key, part):
    source_keys = jax.random.split(jax.random.fold_in(key, 101), DEVICES)
    target_keys = jax.random.split(jax.random.fold_in(key, 202), DEVICES)
    source_perm = jax.vmap(lambda subkey: jax.random.permutation(subkey, LINES_DEV))(source_keys)
    target_perm = jax.vmap(lambda subkey: jax.random.permutation(subkey, LINES_DEV))(target_keys)
    owner_dev = source_perm % DEVICES
    rank_ids = source_perm // DEVICES
    source_ids = jnp.arange(DEVICES, dtype=jnp.int32)[:, None]
    slot_ids = target_perm[owner_dev, source_ids * SENDS + rank_ids]
    return (owner_dev * LINES_DEV + slot_ids).reshape(-1).astype(jnp.int32)


def with_ends(drawn, key, least, high):
    longest = drawn.shape.index(max(drawn.shape))
    spots = []
    for shift in (0, 1):
        where = [jax.random.randint(jax.random.fold_in(key, axis), (), 0, length) for axis, length in enumerate(drawn.shape)]
        where[longest] = (where[longest] + shift) % drawn.shape[longest]
        spots.append(tuple(where))
    return drawn.at[spots[0]].set(least).at[spots[1]].set(high)


def shard_levels(own_key, shape, cuts, low, top_value):
    level, own = 1.0, jax.random.fold_in(own_key, 6)
    for dim, shards_of in cuts:
        draws = jnp.exp(jax.random.uniform(jax.random.fold_in(own, dim), (shards_of,), jnp.float32, low / len(cuts), top_value / len(cuts)))
        level = level * jnp.repeat(draws, shape[dim] // shards_of).reshape([-1 if axis == dim else 1 for axis in range(len(shape))])
    return level


def setup_inputs(seed: int = 0) -> dict:
    key_of = jax.random.split(jax.random.key(seed), 4)
    return {
        "cell_volume": jnp.clip(jnp.exp(math.log(2.0) - 1.3862944 * jax.random.uniform(key_of[0], (NX, NY, NZ), jnp.float32) ** shard_levels(key_of[0], (NX, NY, NZ), ((0, 4), (1, 2), (2, 4)), -0.2, 0.2)), 0.5, 2.0),
        "exponent": with_ends(jax.random.randint(key_of[1], (NX, NY, NZ), 0, 8), jax.random.fold_in(key_of[1], 1), 0, 7).astype(jnp.int32),
        "owner_row": draw_owner_row(jax.random.fold_in(key_of[3], 71), 0),
    }


log_step = 0.3


def reference(cell_volume, exponent, owner_row):
    weight = cell_volume * jnp.exp(-log_step * exponent.astype(jnp.float32))
    current = weight[None, None, None]
    for along in range(3):
        behind = jnp.roll(current, 1, axis=3 + along)
        current = jnp.concatenate([behind, 2.0 * (current + behind), current], axis=along)
    stencil = current.reshape(27, NX, NY, NZ) * 0.015625
    lumped = 1.0 / jnp.sum(stencil, axis=0)
    stencil_lines = stencil.reshape(27, N_GX, EX, N_GY, EY, N_GZ, EZ).transpose(0, 1, 3, 5, 2, 4, 6).reshape(27, LINES, EZ)
    lumped_lines = lumped.reshape(N_GX, EX, N_GY, EY, N_GZ, EZ).transpose(0, 2, 4, 1, 3, 5).reshape(LINES, EZ)
    stencil_out = jnp.zeros((27, LINES, EZ), jnp.float32).at[:, owner_row].set(stencil_lines)
    lumped_out = jnp.zeros((LINES, EZ), jnp.float32).at[owner_row].set(lumped_lines)
    return (stencil_out, lumped_out)
```

```python
import functools

import jax
import jax.numpy as jnp
from jax import lax
from jax.experimental import pallas as pl
from jax.experimental.pallas import tpu as pltpu
from jax.sharding import PartitionSpec as P

MESH = pl.DeviceIdType.MESH
AXES = ("gx", "gy", "gz")
F32, BF16, I32 = jnp.float32, jnp.bfloat16, jnp.int32
log_step = 0.3
NN = (((1,), (0,)), ((), ()))
NT = (((1,), (1,)), ((), ()))


def onehot(mask):
    return jnp.where(mask, 1.0, 0.0).astype(BF16)


def halves(x):
    hi = x.astype(BF16)
    return hi, (x - hi.astype(F32)).astype(BF16)


def pick(sel, x, dims=NN):
    total = None
    for part in halves(x):
        term = lax.dot_general(sel, part, dims, preferred_element_type=F32)
        total = term if total is None else total + term
    return total


def pick_r(x, sel, dims=NN):
    total = None
    for part in halves(x):
        term = lax.dot_general(part, sel, dims, preferred_element_type=F32)
        total = term if total is None else total + term
    return total


def iota(shape, dim):
    return lax.broadcasted_iota(I32, shape, dim)


def roll_lanes(x, shift):
    width = x.shape[1]
    cut = width - shift % width
    return jnp.concatenate([x[:, cut:], x[:, :cut]], axis=1)


def exchange(
    sizes, cv_hbm, ex_hbm, own_hbm, cur_ref, bef_ref,
    cv_ref, ex_ref, own_ref, in_sem,
    sb1, sb2, rb1, rb2, tx, ty, tc, tr, hx, hy, hc, hr,
    s_sem, r_sem, hs_sem, hr_sem, ready,
):
    nx, ny, nz = sizes
    plane = ny * nz
    n = nx * plane
    gx, gy, gz = (lax.axis_index(a) for a in AXES)
    here = gy * nz + gz
    me = gx * plane + here
    sx, sy, width = cv_ref.shape
    lines = sx * sy
    s = lines // n
    spots = [(y, z) for y in range(ny) for z in range(nz)]
    ux, uy, uz = (gx + 1) % nx, (gy + 1) % ny, (gz + 1) % nz
    dx, dy, dz = (gx + nx - 1) % nx, (gy + ny - 1) % ny, (gz + nz - 1) % nz

    def signal(sem, to):
        pl.semaphore_signal(sem, inc=1, device_id=to, device_id_type=MESH)

    def others(visit):
        for y in range(ny):
            for z in range(nz):
                if y or z:
                    visit((gy + y) % ny, (gz + z) % nz)

    scope = jax.named_scope
    with scope("a_in"):
        arrive = []
        for i, (src, dst) in enumerate(((own_hbm, own_ref), (cv_hbm, cv_ref), (ex_hbm, ex_ref))):
            copy = pltpu.make_async_copy(src, dst, in_sem.at[i])
            copy.start()
            arrive.append(copy)
    with scope("b_bar"):
        barrier = pltpu.get_barrier_semaphore()
        others(lambda y, z: signal(barrier, (gx, y, z)))
        corners = [(dy, gz), (gy, dz), (dy, dz)]

        @pl.when(gx > 0)
        def _():
            for y, z in corners:
                signal(barrier, (dx, y, z))

        def greet_below(p, carry):
            signal(barrier, (p, gy, gz))
            return carry

        lax.fori_loop(0, gx, greet_below, 0)

        def greet_above(p, carry):
            for y, z in spots:
                signal(barrier, (p, y, z))
            return carry

        lax.fori_loop(gx + 1, nx, greet_above, 0)
        expect = plane - 1 + gx * plane + (nx - 1 - gx) + jnp.where(gx < nx - 1, len(corners), 0)

    with scope("c_own"):
        arrive[0].wait()
        owner_full = own_ref[...]
        owner = owner_full // lines
        slot = (owner_full % lines).astype(F32)
        mine = owner == iota((n, lines), 0)
        mine_b = onehot(mine)
        below = onehot(iota((lines, lines), 0) < iota((lines, lines), 1))
        counts = lax.dot_general(mine_b, below, NN, preferred_element_type=F32)
        rank = jnp.sum(jnp.where(mine, counts, 0.0), axis=0, keepdims=True).astype(I32)
        place = onehot(owner * s + rank == iota((lines, lines), 0))

        row_id = iota((width, lines), 0)
        at_rank = rank == row_id % s
        group = row_id // s

    with scope("d_inwait"):
        arrive[1].wait()
        arrive[2].wait()
    with scope("e_pack0"):
        w3 = cv_ref[...] * jnp.exp(-log_step * ex_ref[...].astype(F32))
        w = w3.reshape(lines, width)
        tx[...] = w[lines - sy :, :]
        ty[...] = w3[:, sy - 1 :, :]
        tc[...] = w[lines - 1 :, :]
        last = onehot(iota((8, width), 1) == width - 1)
        tr[...] = pick(last, w, NT)[0:1, :]
        sb1[...] = pick(place, w).reshape(n, s, width)

    with scope("g_barwait"):
        pl.semaphore_wait(barrier, expect)
        others(lambda y, z: signal(ready, (gx, y, z)))

    with scope("h_halosend"):
        halo = []
        routes = [
            (tx, hx, (ux, gy, gz)),
            (ty, hy, (gx, uy, gz)),
            (tc, hc, (ux, uy, gz)),
            (tr, hr.at[0], (gx, gy, uz)),
            (tr, hr.at[1], (ux, gy, uz)),
            (tr, hr.at[2], (gx, uy, uz)),
            (tr, hr.at[3], (ux, uy, uz)),
        ]
        for i, (src, dst, to) in enumerate(routes):
            copy = pltpu.make_async_remote_copy(
                src_ref=src, dst_ref=dst, send_sem=hs_sem.at[i], recv_sem=hr_sem.at[i],
                device_id=to, device_id_type=MESH,
            )
            copy.start()
            halo.append(copy)

    def send_one(stage, sb, rb, p, y, z):
        pltpu.make_async_remote_copy(
            src_ref=sb.at[p * plane + y * nz + z], dst_ref=rb.at[me], send_sem=s_sem.at[stage], recv_sem=r_sem.at[stage],
            device_id=(p, y, z), device_id_type=MESH,
        ).start()

    def send_below(stage, sb, rb):
        def send(p, carry):
            for y, z in spots:
                send_one(stage, sb, rb, p, y, z)
            return carry

        lax.fori_loop(0, gx, send, 0)

    def send_above(stage, sb, rb):
        def send(k, carry):
            for y, z in spots:
                send_one(stage, sb, rb, nx - 1 - k, y, z)
            return carry

        lax.fori_loop(0, nx - 1 - gx, send, 0)

    def send_plane(stage, sb, rb):
        others(lambda y, z: send_one(stage, sb, rb, gx, y, z))
        pltpu.make_async_copy(sb.at[me], rb.at[me], r_sem.at[stage]).start()

    with scope("i_send0"):
        send_below(0, sb1, rb1)
        send_plane(0, sb1, rb1)
    with scope("j_ready"):
        pl.semaphore_wait(ready, plane - 1)
    with scope("k_send0"):
        send_above(0, sb1, rb1)

    with scope("l_halo"):
        for copy in halo:
            copy.wait()

    with scope("m_pack1"):
        line_id = iota((lines, width), 0)
        first_j = line_id % sy == 0

        def back_j(x, edge):
            edge_full = jnp.broadcast_to(edge, (sx, sy, width)).reshape(lines, width)
            shifted = jnp.concatenate([x[lines - 1 :, :], x[: lines - 1, :]], axis=0)
            return jnp.where(first_j, edge_full, shifted)

        edge = hy[...]
        x1 = jnp.concatenate([hx[...], w[: lines - sy, :]], axis=0)
        x2 = back_j(w, edge)
        x3 = back_j(x1, jnp.concatenate([hc[...].reshape(1, 1, width), edge[: sx - 1]], axis=0))
        for c, x in enumerate((x1, x2, x3)):
            sb2[:, c * s : (c + 1) * s, :] = pick(place, x).reshape(n, s, width)

        lane = iota((1, lines), 1)
        at_j0 = lane % sy == 0
        r0, rx, ry, rxy = hr[0], hr[1], hr[2], hr[3]
        rim1 = jnp.where(lane < sy, roll_lanes(rx, sy), roll_lanes(r0, sy))
        rim2 = jnp.where(at_j0, roll_lanes(ry, 1 - sy), roll_lanes(r0, 1))
        edge_rim = jnp.where(lane == 0, roll_lanes(rxy, 1), roll_lanes(ry, 1))
        rim3 = jnp.where(at_j0, edge_rim, roll_lanes(rim1, 1))
        rims = slot
        for q, rim in enumerate((r0, rim1, rim2, rim3)):
            rims = jnp.where(group == q, rim, rims)
        rims = jnp.where(at_rank & (group < 5), rims, 0.0)
        sb2[:, 3 * s : 3 * s + 1, :] = pick(mine_b, rims, NT).reshape(n, 1, width)

    with scope("n_send1"):
        send_below(1, sb2, rb2)
        send_above(1, sb2, rb2)
        send_plane(1, sb2, rb2)

    with scope("q_wait"):
        pltpu.make_async_copy(rb1, rb1, r_sem.at[0]).wait()
        pltpu.make_async_copy(rb2, rb2, r_sem.at[1]).wait()
    with scope("r_unp"):
        extra = rb2[:, 3 * s : 3 * s + 1, :]
        spread = jnp.broadcast_to(extra, (n, s, width)).reshape(lines, width)
        spread = jnp.where(iota((lines, width), 1) % s == iota((lines, width), 0) % s, spread, 0.0)
        sums = onehot(iota((8, width), 1) // s == iota((8, width), 0))
        rows = pick(sums, spread, NT)
        to_slot = onehot(rows[4:5, :].astype(I32) == iota((lines, lines), 0))
        cur_ref[0] = pick(to_slot, rb1[...].reshape(lines, width))
        for c in range(3):
            cur_ref[c + 1] = pick(to_slot, rb2[:, c * s : (c + 1) * s, :].reshape(lines, width))
        bef_ref[...] = pick(to_slot, jnp.concatenate([rows, jnp.zeros((width - 8, lines), F32)], axis=0), NT)

    with scope("w_drain"):
        for stage, sb in enumerate((sb1, sb2)):
            sent = sb.at[pl.ds(0, n - 1)]
            pltpu.make_async_copy(sent, sent, s_sem.at[stage]).wait()


def finish(cur_ref, bef_ref, out_ref, lump_ref):
    shape = cur_ref.shape[1:]
    at_0 = iota(shape, 1) == 0
    near, far = [], []
    for c in range(4):
        x = cur_ref[c] * 0.015625
        shifted = pltpu.roll(x, 1, axis=1)
        near.append(x)
        far.append(jnp.where(at_0, bef_ref[:, c : c + 1] * 0.015625, shifted))

    def triple(c, b):
        return (b, 2.0 * (c + b), c)

    def nine(v):
        by_x0 = triple(v[0], v[1])
        by_x1 = triple(v[2], v[3])
        return [triple(by_x0[o1], by_x1[o1]) for o1 in range(3)]

    cur, back = nine(near), nine(far)
    for o1 in range(3):
        for o2 in range(3):
            for o3, value in enumerate(triple(cur[o1][o2], back[o1][o2])):
                out_ref[9 * o1 + 3 * o2 + o3] = value
    total = functools.reduce(lambda a, b: a + b, near + far)
    lump_ref[...] = 1.0 / (27.0 * total)


def shards(sizes, cell_volume, exponent, owner_row):
    sx, sy, width = cell_volume.shape
    lines = sx * sy
    n = sizes[0] * sizes[1] * sizes[2]
    s = lines // n
    vmem = pl.BlockSpec(memory_space=pltpu.VMEM)
    dma = pltpu.SemaphoreType.DMA
    cur, bef = pl.pallas_call(
        functools.partial(exchange, sizes),
        out_shape=(
            jax.ShapeDtypeStruct((4, lines, width), F32),
            jax.ShapeDtypeStruct((lines, width), F32),
        ),
        in_specs=[pl.BlockSpec(memory_space=pltpu.HBM)] * 3,
        out_specs=(vmem, vmem),
        scratch_shapes=[
            pltpu.VMEM((sx, sy, width), F32),
            pltpu.VMEM((sx, sy, width), I32),
            pltpu.VMEM((1, lines), I32),
            dma((3,)),
        ]
        + [pltpu.VMEM((n, rows, width), F32) for rows in (s, 3 * s + 1)] * 2
        + [
            pltpu.VMEM((sy, width), F32),
            pltpu.VMEM((sx, 1, width), F32),
            pltpu.VMEM((1, width), F32),
            pltpu.VMEM((1, lines), F32),
            pltpu.VMEM((sy, width), F32),
            pltpu.VMEM((sx, 1, width), F32),
            pltpu.VMEM((1, width), F32),
            pltpu.VMEM((4, 1, lines), F32),
            dma((2,)),
            dma((2,)),
            dma((7,)),
            dma((7,)),
            pltpu.SemaphoreType.REGULAR,
        ],
        compiler_params=pltpu.CompilerParams(
            collective_id=0, has_side_effects=True, vmem_limit_bytes=16 << 20
        ),
    )(*(pltpu.with_memory_space_constraint(a, pltpu.HBM) for a in (cell_volume, exponent, owner_row.reshape(1, lines))))
    rows = 128
    return pl.pallas_call(
        finish,
        grid=(lines // rows,),
        out_shape=(
            jax.ShapeDtypeStruct((27, lines, width), F32),
            jax.ShapeDtypeStruct((lines, width), F32),
        ),
        in_specs=[
            pl.BlockSpec((4, rows, width), lambda i: (0, i, 0)),
            pl.BlockSpec((rows, width), lambda i: (i, 0)),
        ],
        out_specs=(
            pl.BlockSpec((27, rows, width), lambda i: (0, i, 0)),
            pl.BlockSpec((rows, width), lambda i: (i, 0)),
        ),
        compiler_params=pltpu.CompilerParams(vmem_limit_bytes=16 << 20),
    )(cur, bef)


def solution(mesh):
    sizes = tuple(mesh.shape[a] for a in AXES)
    return jax.shard_map(
        functools.partial(shards, sizes),
        mesh=mesh,
        in_specs=(P(*AXES), P(*AXES), P(AXES)),
        out_specs=(P(None, AXES, None), P(AXES, None)),
        check_vma=False,
    )
```

```python
import functools

import jax
import jax.numpy as jnp
from jax import lax
from jax.experimental import pallas as pl
from jax.experimental.pallas import tpu as pltpu
from jax.sharding import PartitionSpec as P

MESH = pl.DeviceIdType.MESH
AXES = ("gx", "gy", "gz")
F32, BF16, I32 = jnp.float32, jnp.bfloat16, jnp.int32
log_step = 0.3
NN = (((1,), (0,)), ((), ()))
NT = (((1,), (1,)), ((), ()))


def onehot(mask):
    return jnp.where(mask, 1.0, 0.0).astype(BF16)


def halves(x):
    hi = x.astype(BF16)
    return hi, (x - hi.astype(F32)).astype(BF16)


def pick(sel, x, dims=NN):
    total = None
    for part in halves(x):
        term = lax.dot_general(sel, part, dims, preferred_element_type=F32)
        total = term if total is None else total + term
    return total


def pick_r(x, sel, dims=NN):
    total = None
    for part in halves(x):
        term = lax.dot_general(part, sel, dims, preferred_element_type=F32)
        total = term if total is None else total + term
    return total


def iota(shape, dim):
    return lax.broadcasted_iota(I32, shape, dim)


def roll_lanes(x, shift):
    width = x.shape[1]
    cut = width - shift % width
    return jnp.concatenate([x[:, cut:], x[:, :cut]], axis=1)


def exchange(
    sizes, cv_hbm, ex_hbm, own_hbm, rb1, rb2,
    cv_ref, ex_ref, own_ref, in_sem,
    sb1, sb2, tx, ty, tc, tr, hx, hy, hc, hr,
    s_sem, r_sem, hs_sem, hr_sem, ready,
    vb1, vb2, wv, raw, raw_own, vx, vy, vc, vr, vs_sem, vr_sem,
):
    nx, ny, nz = sizes
    plane = ny * nz
    n = nx * plane
    gx, gy, gz = (lax.axis_index(a) for a in AXES)
    here = gy * nz + gz
    me = gx * plane + here
    sx, sy, width = cv_ref.shape
    lines = sx * sy
    s = lines // n
    relay = nx == 4
    half = n // 2
    base = (gx // 2) * 2
    middle = (gx == 1) | (gx == 2)
    across = (gx + 2) % nx
    theirs = across * plane + here
    spots = [(y, z) for y in range(ny) for z in range(nz)]
    ux, uy, uz = (gx + 1) % nx, (gy + 1) % ny, (gz + 1) % nz
    dx, dy, dz = (gx + nx - 1) % nx, (gy + ny - 1) % ny, (gz + nz - 1) % nz

    def signal(sem, to):
        pl.semaphore_signal(sem, inc=1, device_id=to, device_id_type=MESH)

    def others(visit):
        for y in range(ny):
            for z in range(nz):
                if y or z:
                    visit((gy + y) % ny, (gz + z) % nz)

    scope = jax.named_scope
    with scope("a_in"):
        arrive = []
        for i, (src, dst) in enumerate(((own_hbm, own_ref), (cv_hbm, cv_ref), (ex_hbm, ex_ref))):
            copy = pltpu.make_async_copy(src, dst, in_sem.at[i])
            copy.start()
            arrive.append(copy)
    with scope("b_bar"):
        barrier = pltpu.get_barrier_semaphore()
        others(lambda y, z: signal(barrier, (gx, y, z)))
        corners = [(dy, gz), (gy, dz), (dy, dz)]

        @pl.when(gx > 0)
        def _():
            for y, z in corners:
                signal(barrier, (dx, y, z))

        def greet_below(p, carry):
            signal(barrier, (p, gy, gz))
            return carry

        reach = 2 if relay else nx
        lax.fori_loop(jnp.maximum(gx - reach, 0), gx, greet_below, 0)

        def greet_above(p, carry):
            for y, z in spots:
                signal(barrier, (p, y, z))
            return carry

        lax.fori_loop(gx + 1, nx, greet_above, 0)
        expect = plane - 1 + gx * plane + jnp.minimum(nx - 1 - gx, reach) + jnp.where(gx < nx - 1, len(corners), 0)

    with scope("c_own"):
        arrive[0].wait()
        def ranks(own):
            owner = own // lines
            mine = owner == iota((n, lines), 0)
            counts = lax.dot_general(onehot(mine), below, NN, preferred_element_type=F32)
            rank = jnp.sum(jnp.where(mine, counts, 0.0), axis=0, keepdims=True).astype(I32)
            return onehot(mine), rank, owner * s + rank, (own % lines).astype(F32)

        below = onehot(iota((lines, lines), 0) < iota((lines, lines), 1))
        mine_b, rank, goes, slot = ranks(own_ref[...])
        place = onehot(goes == iota((lines, lines), 0))
        row_id = iota((width, lines), 0)
        group = row_id // s

    with scope("d_inwait"):
        arrive[1].wait()
        arrive[2].wait()
    with scope("e_pack0"):
        w3 = cv_ref[...] * jnp.exp(-log_step * ex_ref[...].astype(F32))
        w = w3.reshape(lines, width)
        wv[...] = w
        tx[...] = w[lines - sy :, :]
        ty[...] = w3[:, sy - 1 :, :]
        tc[...] = w[lines - 1 :, :]
        last = onehot(iota((8, width), 1) == width - 1)
        tr[...] = pick(last, w, NT)[0:1, :]
        sb1[...] = pick(place, w).reshape(n, s, width)

    with scope("g_barwait"):
        pl.semaphore_wait(barrier, expect)
        others(lambda y, z: signal(ready, (gx, y, z)))

    with scope("h_halosend"):
        halo = []
        routes = [
            (tx, hx, (ux, gy, gz)),
            (ty, hy, (gx, uy, gz)),
            (tc, hc, (ux, uy, gz)),
            (tr, hr.at[0], (gx, gy, uz)),
            (tr, hr.at[1], (ux, gy, uz)),
            (tr, hr.at[2], (gx, uy, uz)),
            (tr, hr.at[3], (ux, uy, uz)),
        ]
        for i, (src, dst, to) in enumerate(routes):
            copy = pltpu.make_async_remote_copy(
                src_ref=src, dst_ref=dst, send_sem=hs_sem.at[i], recv_sem=hr_sem.at[i],
                device_id=to, device_id_type=MESH,
            )
            copy.start()
            halo.append(copy)

    def hand(i, src, dst, to):
        return pltpu.make_async_remote_copy(
            src_ref=src, dst_ref=dst, send_sem=vs_sem.at[i], recv_sem=vr_sem.at[i], device_id=to, device_id_type=MESH
        )

    back = jnp.maximum(gx - 1, 0)
    raw_copies = [
        hand(1, own_ref, raw_own, (across, gy, gz)),
        hand(0, wv, raw, (across, gy, gz)),
    ]
    back_copies = [
        hand(2, tx, vx, (back, gy, gz)),
        hand(3, tc, vc, (back, uy, gz)),
        hand(4, tr, vr.at[1], (back, gy, uz)),
        hand(5, tr, vr.at[3], (back, uy, uz)),
    ]
    side_copies = [
        hand(6, ty, vy, (across, uy, gz)),
        hand(7, tr, vr.at[0], (across, gy, uz)),
        hand(8, tr, vr.at[2], (across, uy, uz)),
    ]

    def start_when(flag, copies):
        @pl.when(flag)
        def _():
            for copy in copies:
                copy.start()

    if relay:
        with scope("h_raw"):
            start_when(gx >= 2, back_copies)
            start_when(gx == nx - 1, side_copies + raw_copies)

    def send_one(stage, sb, rb, p, y, z):
        pltpu.make_async_remote_copy(
            src_ref=sb.at[p * plane + y * nz + z], dst_ref=rb.at[me], send_sem=s_sem.at[stage], recv_sem=r_sem.at[stage],
            device_id=(p, y, z), device_id_type=MESH,
        ).start()

    low, top = 0, nx - 1
    if relay:
        low, top = jnp.where(middle, 0, base), jnp.where(middle, nx - 1, base + 1)

    def send_below(stage, sb, rb):
        def send(p, carry):
            for y, z in spots:
                send_one(stage, sb, rb, p, y, z)
            return carry

        lax.fori_loop(low, gx, send, 0)

    def send_above(stage, sb, rb):
        def send(k, carry):
            for y, z in spots:
                send_one(stage, sb, rb, top - k, y, z)
            return carry

        lax.fori_loop(0, top - gx, send, 0)

    def send_plane(stage, sb, rb):
        others(lambda y, z: send_one(stage, sb, rb, gx, y, z))
        pltpu.make_async_copy(sb.at[me], rb.at[me], r_sem.at[stage]).start()

    with scope("i_send0"):
        send_below(0, sb1, rb1)
        send_plane(0, sb1, rb1)
    with scope("j_ready"):
        pl.semaphore_wait(ready, plane - 1)
    with scope("k_send0"):
        if relay:
            start_when(gx == 0, side_copies + raw_copies)
        send_above(0, sb1, rb1)

    with scope("l_halo"):
        for copy in halo:
            copy.wait()

    with scope("m_pack1"):
        line_id = iota((lines, width), 0)
        first_j = line_id % sy == 0
        lane = iota((1, lines), 1)
        at_j0 = lane % sy == 0

        def back_j(x, edge):
            edge_full = jnp.broadcast_to(edge, (sx, sy, width)).reshape(lines, width)
            shifted = jnp.concatenate([x[lines - 1 :, :], x[: lines - 1, :]], axis=0)
            return jnp.where(first_j, edge_full, shifted)

        def neighbours(w, hx, hy, hc):
            edge = hy[...]
            x1 = jnp.concatenate([hx[...], w[: lines - sy, :]], axis=0)
            x2 = back_j(w, edge)
            x3 = back_j(x1, jnp.concatenate([hc[...].reshape(1, 1, width), edge[: sx - 1]], axis=0))
            return x1, x2, x3

        def rim_rows(hr, mine_b, rank, slot):
            r0, rx, ry, rxy = hr[0], hr[1], hr[2], hr[3]
            rim1 = jnp.where(lane < sy, roll_lanes(rx, sy), roll_lanes(r0, sy))
            rim2 = jnp.where(at_j0, roll_lanes(ry, 1 - sy), roll_lanes(r0, 1))
            edge_rim = jnp.where(lane == 0, roll_lanes(rxy, 1), roll_lanes(ry, 1))
            rim3 = jnp.where(at_j0, edge_rim, roll_lanes(rim1, 1))
            rims = slot
            for q, rim in enumerate((r0, rim1, rim2, rim3)):
                rims = jnp.where(group == q, rim, rims)
            rims = jnp.where((rank == row_id % s) & (group < 5), rims, 0.0)
            return pick(mine_b, rims, NT)

        for c, x in enumerate(neighbours(w, hx, hy, hc)):
            sb2[:, c * s : (c + 1) * s, :] = pick(place, x).reshape(n, s, width)
        sb2[:, 3 * s : 3 * s + 1, :] = rim_rows(hr, mine_b, rank, slot).reshape(n, 1, width)

    with scope("n_send1"):
        send_below(1, sb2, rb2)
        send_above(1, sb2, rb2)
        send_plane(1, sb2, rb2)

    def send_theirs(stage, sb, rb):
        end = jnp.where(gx == 1, 0, nx - 1)

        def to(p, y, z):
            pltpu.make_async_remote_copy(
                src_ref=sb.at[(p - base) * plane + y * nz + z], dst_ref=rb.at[theirs],
                send_sem=vs_sem.at[9 + stage], recv_sem=r_sem.at[stage],
                device_id=(p, y, z), device_id_type=MESH,
            ).start()

        for y, z in spots:
            to(end, y, z)
        others(lambda y, z: to(gx, y, z))
        pltpu.make_async_copy(sb.at[(gx - base) * plane + here], rb.at[theirs], r_sem.at[stage]).start()

    if relay:

        @pl.when(middle)
        def _():
            with scope("o_wait0"):
                for copy in back_copies + side_copies:
                    copy.wait_recv()
                raw_copies[0].wait_recv()
            with scope("o_prep"):
                _, rank_v, goes_v, slot_v = ranks(raw_own[...])
                place_v = onehot(goes_v - base * plane * s == iota((lines // 2, lines), 0))
                mine_v = onehot(raw_own[...] // lines - base * plane == iota((half, lines), 0))
                vb2[:, 3 * s : 3 * s + 1, :] = rim_rows(vr, mine_v, rank_v, slot_v).reshape(half, 1, width)
            with scope("o_wait1"):
                raw_copies[1].wait_recv()
            with scope("o_pack"):
                x0 = raw[...]
                vb1[...] = pick(place_v, x0).reshape(half, s, width)
                for c, x in enumerate(neighbours(x0, vx, vy, vc)):
                    vb2[:, c * s : (c + 1) * s, :] = pick(place_v, x).reshape(half, s, width)
            with scope("o_send"):
                send_theirs(0, vb1, rb1)
                send_theirs(1, vb2, rb2)

    with scope("q_wait"):
        pltpu.make_async_copy(rb1, rb1, r_sem.at[0]).wait()
        pltpu.make_async_copy(rb2, rb2, r_sem.at[1]).wait()
    with scope("w_drain"):
        def sent(sb, count, sem):
            done = sb.at[pl.ds(0, count)]
            pltpu.make_async_copy(done, done, sem).wait()

        def drain(count):
            for stage, sb in enumerate((sb1, sb2)):
                sent(sb, count, s_sem.at[stage])

        if relay:

            @pl.when(middle)
            def _():
                drain(n - 1)
                for stage, sb in enumerate((vb1, vb2)):
                    sent(sb, half - 1, vs_sem.at[9 + stage])

            @pl.when(jnp.logical_not(middle))
            def _():
                drain(half - 1)
                for copy in raw_copies + side_copies:
                    copy.wait_send()

            @pl.when(gx >= 2)
            def _():
                for copy in back_copies:
                    copy.wait_send()

        else:
            drain(n - 1)


def finish(n, parts, rb1, rb2, out_hbm, lump_hbm, cur, bef, out_ref, lump_ref, sem):
    lines, width = lump_ref.shape
    s = lines // n
    extra = rb2[:, 3 * s : 3 * s + 1, :]
    spread = jnp.broadcast_to(extra, (n, s, width)).reshape(lines, width)
    spread = jnp.where(iota((lines, width), 1) % s == iota((lines, width), 0) % s, spread, 0.0)
    sums = onehot(iota((8, width), 1) // s == iota((8, width), 0))
    rows = pick(sums, spread, NT)
    slot = rows[4:5, :].astype(I32)
    rims = halves(jnp.concatenate([rows, jnp.zeros((width - 8, lines), F32)], axis=0))
    got = [halves(rb1[...].reshape(lines, width) * 0.015625)]
    got += [halves(rb2[:, c * s : (c + 1) * s, :].reshape(lines, width) * 0.015625) for c in range(3)]

    def triple(c, b):
        return (b, 2.0 * (c + b), c)

    def nine(v):
        by_x0 = triple(v[0], v[1])
        by_x1 = triple(v[2], v[3])
        return [triple(by_x0[o1], by_x1[o1]) for o1 in range(3)]

    def copies(first, count):
        part = pl.ds(first, count)
        return (
            pltpu.make_async_copy(out_ref.at[:, part, :], out_hbm.at[:, part, :], sem),
            pltpu.make_async_copy(lump_ref.at[part, :], lump_hbm.at[part, :], sem),
        )

    first = 0
    for count, piece in parts:
        to_slot = onehot(slot == iota((count, lines), 0) + first)
        for c in range(4):
            hi, lo = got[c]
            cur[c, first : first + count, :] = lax.dot_general(to_slot, hi, NN, preferred_element_type=F32) + lax.dot_general(
                to_slot, lo, NN, preferred_element_type=F32
            )
        hi, lo = rims
        bef[first : first + count, :] = lax.dot_general(to_slot, hi, NT, preferred_element_type=F32) + lax.dot_general(
            to_slot, lo, NT, preferred_element_type=F32
        )
        for start in range(first, first + count, piece):
            span = slice(start, start + piece)
            at_0 = iota((piece, width), 1) == 0
            near, far = [], []
            for c in range(4):
                x = cur[c, span, :]
                near.append(x)
                far.append(jnp.where(at_0, bef[span, c : c + 1] * 0.015625, pltpu.roll(x, 1, axis=1)))
            ahead, back = nine(near), nine(far)
            for o1 in range(3):
                for o2 in range(3):
                    for o3, value in enumerate(triple(ahead[o1][o2], back[o1][o2])):
                        out_ref[9 * o1 + 3 * o2 + o3, span, :] = value
            total = functools.reduce(lambda a, b: a + b, near + far)
            lump_ref[span, :] = 1.0 / (27.0 * total)
            for copy in copies(start, piece):
                copy.start()
        first += count
    for copy in copies(0, lines):
        copy.wait()


def shards(sizes, cell_volume, exponent, owner_row):
    sx, sy, width = cell_volume.shape
    lines = sx * sy
    n = sizes[0] * sizes[1] * sizes[2]
    s = lines // n
    vmem = pl.BlockSpec(memory_space=pltpu.VMEM)
    dma = pltpu.SemaphoreType.DMA
    rb1, rb2 = pl.pallas_call(
        functools.partial(exchange, sizes),
        out_shape=(
            jax.ShapeDtypeStruct((n, s, width), F32),
            jax.ShapeDtypeStruct((n, 3 * s + 1, width), F32),
        ),
        in_specs=[pl.BlockSpec(memory_space=pltpu.HBM)] * 3,
        out_specs=(vmem, vmem),
        scratch_shapes=[
            pltpu.VMEM((sx, sy, width), F32),
            pltpu.VMEM((sx, sy, width), I32),
            pltpu.VMEM((1, lines), I32),
            dma((3,)),
        ]
        + [pltpu.VMEM((n, rows, width), F32) for rows in (s, 3 * s + 1)]
        + [
            pltpu.VMEM((sy, width), F32),
            pltpu.VMEM((sx, 1, width), F32),
            pltpu.VMEM((1, width), F32),
            pltpu.VMEM((1, lines), F32),
            pltpu.VMEM((sy, width), F32),
            pltpu.VMEM((sx, 1, width), F32),
            pltpu.VMEM((1, width), F32),
            pltpu.VMEM((4, 1, lines), F32),
            dma((2,)),
            dma((2,)),
            dma((7,)),
            dma((7,)),
            pltpu.SemaphoreType.REGULAR,
        ]
        + [pltpu.VMEM((n // 2, rows, width), F32) for rows in (s, 3 * s + 1)]
        + [
            pltpu.VMEM((lines, width), F32),
            pltpu.VMEM((lines, width), F32),
            pltpu.VMEM((1, lines), I32),
            pltpu.VMEM((sy, width), F32),
            pltpu.VMEM((sx, 1, width), F32),
            pltpu.VMEM((1, width), F32),
            pltpu.VMEM((4, 1, lines), F32),
            dma((11,)),
            dma((9,)),
        ],
        compiler_params=pltpu.CompilerParams(
            collective_id=0, has_side_effects=True, vmem_limit_bytes=16 << 20
        ),
    )(*(pltpu.with_memory_space_constraint(a, pltpu.HBM) for a in (cell_volume, exponent, owner_row.reshape(1, lines))))
    parts = [(lines // 4, lines // 8)] * 4
    return pl.pallas_call(
        functools.partial(finish, n, parts),
        out_shape=(
            jax.ShapeDtypeStruct((27, lines, width), F32),
            jax.ShapeDtypeStruct((lines, width), F32),
        ),
        in_specs=[vmem, vmem],
        out_specs=(pl.BlockSpec(memory_space=pltpu.HBM), pl.BlockSpec(memory_space=pltpu.HBM)),
        scratch_shapes=[
            pltpu.VMEM((4, lines, width), F32),
            pltpu.VMEM((lines, width), F32),
            pltpu.VMEM((27, lines, width), F32),
            pltpu.VMEM((lines, width), F32),
            dma,
        ],
        compiler_params=pltpu.CompilerParams(vmem_limit_bytes=16 << 20),
    )(rb1, rb2)


def solution(mesh):
    sizes = tuple(mesh.shape[a] for a in AXES)
    return jax.shard_map(
        functools.partial(shards, sizes),
        mesh=mesh,
        in_specs=(P(*AXES), P(*AXES), P(AXES)),
        out_specs=(P(None, AXES, None), P(AXES, None)),
        check_vma=False,
    )
```

```python
import functools

import jax
import jax.numpy as jnp
from jax import lax
from jax.experimental import pallas as pl
from jax.experimental.pallas import tpu as pltpu
from jax.sharding import PartitionSpec as P

MESH = pl.DeviceIdType.MESH
AXES = ("gx", "gy", "gz")
F32, BF16, I32 = jnp.float32, jnp.bfloat16, jnp.int32
log_step = 0.3
NN = (((1,), (0,)), ((), ()))
NT = (((1,), (1,)), ((), ()))


def onehot(mask):
    return jnp.where(mask, 1.0, 0.0).astype(BF16)


def halves(x):
    hi = x.astype(BF16)
    return hi, (x - hi.astype(F32)).astype(BF16)


def pick(sel, x, dims=NN):
    total = None
    for part in halves(x):
        term = lax.dot_general(sel, part, dims, preferred_element_type=F32)
        total = term if total is None else total + term
    return total


def pick_r(x, sel, dims=NN):
    total = None
    for part in halves(x):
        term = lax.dot_general(part, sel, dims, preferred_element_type=F32)
        total = term if total is None else total + term
    return total


def iota(shape, dim):
    return lax.broadcasted_iota(I32, shape, dim)


def roll_lanes(x, shift):
    width = x.shape[1]
    cut = width - shift % width
    return jnp.concatenate([x[:, cut:], x[:, :cut]], axis=1)


def exchange(
    sizes, cv_hbm, ex_hbm, own_hbm, rb1, rb2,
    cv_ref, ex_ref, own_ref, in_sem,
    sb1, sb2, tx, ty, tc, tr, hx, hy, hc, hr,
    s_sem, r_sem, h_sem, v_sem, ready,
    vb1, vb2, wv, raw, raw_own, vx, vy, vc, vr, tally,
):
    nx, ny, nz = sizes
    plane = ny * nz
    n = nx * plane
    gx, gy, gz = (lax.axis_index(a) for a in AXES)
    here = gy * nz + gz
    me = gx * plane + here
    sx, sy, width = cv_ref.shape
    lines = sx * sy
    s = lines // n
    relay = nx == 4
    half = n // 2
    base = (gx // 2) * 2
    middle = (gx == 1) | (gx == 2)
    across, beside = (gx + 2) % nx, jnp.where(gx < 2, 1 - gx, nx + 1 - gx)
    give, take = jnp.where(middle, beside, across), jnp.where(middle, across, beside)
    theirs = take * plane + here
    spots = [(y, z) for y in range(ny) for z in range(nz)]
    ux, uy, uz = (gx + 1) % nx, (gy + 1) % ny, (gz + 1) % nz
    dx, dy, dz = (gx + nx - 1) % nx, (gy + ny - 1) % ny, (gz + nz - 1) % nz

    def signal(sem, to):
        pl.semaphore_signal(sem, inc=1, device_id=to, device_id_type=MESH)

    def others(visit):
        for y in range(ny):
            for z in range(nz):
                if y or z:
                    visit((gy + y) % ny, (gz + z) % nz)

    def done(rows, sem):
        part = tally.at[pl.ds(0, rows)]
        pltpu.make_async_copy(part, part, sem).wait()

    edge_rows = sx + sy + 1 + 4 * lines // width
    pair_rows = 4 * s + 1

    scope = jax.named_scope
    with scope("a_in"):
        arrive = []
        for i, (src, dst) in enumerate(((own_hbm, own_ref), (cv_hbm, cv_ref), (ex_hbm, ex_ref))):
            copy = pltpu.make_async_copy(src, dst, in_sem.at[min(i, 1)])
            copy.start()
            arrive.append(copy)
    with scope("b_bar"):
        barrier = pltpu.get_barrier_semaphore()
        others(lambda y, z: signal(barrier, (gx, y, z)))
        corners = [(dy, gz), (gy, dz), (dy, dz)]

        @pl.when(gx > 0)
        def _():
            for y, z in corners:
                signal(barrier, (dx, y, z))

        def greet_below(p, carry):
            signal(barrier, (p, gy, gz))
            return carry

        reach = 2 if relay else nx
        lax.fori_loop(jnp.maximum(gx - reach, 0), gx, greet_below, 0)

        def greet_above(p, carry):
            if relay:

                @pl.when(p == 1)
                def _():
                    signal(barrier, (p, gy, gz))

                @pl.when(p > 1)
                def _():
                    for y, z in spots:
                        signal(barrier, (p, y, z))
            else:
                for y, z in spots:
                    signal(barrier, (p, y, z))
            return carry

        lax.fori_loop(gx + 1, nx, greet_above, 0)
        expect = plane - 1 + gx * plane + jnp.minimum(nx - 1 - gx, reach) + jnp.where(gx < nx - 1, len(corners), 0)
        if relay:
            expect -= jnp.where(gx == 1, plane - 1, 0)

    with scope("c_own"):
        arrive[0].wait()
        def ranks(own):
            owner = own // lines
            mine = owner == iota((n, lines), 0)
            counts = lax.dot_general(onehot(mine), below, NN, preferred_element_type=F32)
            rank = jnp.sum(jnp.where(mine, counts, 0.0), axis=0, keepdims=True).astype(I32)
            return onehot(mine), rank, owner * s + rank, (own % lines).astype(F32)

        below = onehot(iota((lines, lines), 0) < iota((lines, lines), 1))
        mine_b, rank, goes, slot = ranks(own_ref[...])
        place = onehot(goes == iota((lines, lines), 0))
        row_id = iota((width, lines), 0)
        group = row_id // s

    with scope("d_inwait"):
        done(2 * lines, in_sem.at[1])
    with scope("e_pack0"):
        w3 = cv_ref[...] * jnp.exp(-log_step * ex_ref[...].astype(F32))
        w = w3.reshape(lines, width)
        wv[...] = w
        tx[...] = w[lines - sy :, :]
        ty[...] = w3[:, sy - 1 :, :]
        tc[...] = w[lines - 1 :, :]
        last = onehot(iota((8, width), 1) == width - 1)
        tr[...] = pick(last, w, NT)[0:1, :]
        sb1[...] = pick(place, w).reshape(n, s, width)

    with scope("g_barwait"):
        pl.semaphore_wait(barrier, expect)
        others(lambda y, z: signal(ready, (gx, y, z)))

    with scope("h_halosend"):
        routes = [
            (tx, hx, (ux, gy, gz)),
            (ty, hy, (gx, uy, gz)),
            (tc, hc, (ux, uy, gz)),
            (tr, hr.at[0], (gx, gy, uz)),
            (tr, hr.at[1], (ux, gy, uz)),
            (tr, hr.at[2], (gx, uy, uz)),
            (tr, hr.at[3], (ux, uy, uz)),
        ]
        for i, (src, dst, to) in enumerate(routes):
            copy = pltpu.make_async_remote_copy(
                src_ref=src, dst_ref=dst, send_sem=s_sem, recv_sem=h_sem,
                device_id=to, device_id_type=MESH,
            )
            copy.start()

    def hand(sem, src, dst):
        return pltpu.make_async_remote_copy(
            src_ref=src, dst_ref=dst, send_sem=s_sem, recv_sem=sem, device_id=(give, gy, gz), device_id_type=MESH
        )

    raw_copies = [hand(v_sem.at[0], own_ref, raw_own), hand(v_sem.at[1], wv, raw)]
    edge_copies = [hand(v_sem.at[0], src, dst) for src, dst in ((hx, vx), (hy, vy), (hc, vc), (hr, vr))]

    def start_when(flag, copies):
        @pl.when(flag)
        def _():
            for copy in copies:
                copy.start()

    if relay:
        with scope("h_raw"):
            start_when(gx > 0, raw_copies)

    def send_one(stage, sb, rb, p, y, z):
        pltpu.make_async_remote_copy(
            src_ref=sb.at[p * plane + y * nz + z], dst_ref=rb.at[me], send_sem=s_sem, recv_sem=r_sem,
            device_id=(p, y, z), device_id_type=MESH,
        ).start()

    low, top = 0, nx - 1
    if relay:
        low = jnp.where(gx == 2, 0, jnp.where(gx == 1, 1, base))
        top = jnp.where(gx == 1, nx - 1, jnp.where(gx == 2, 2, base + 1))

    def send_below(stage, sb, rb):
        def send(p, carry):
            for y, z in spots:
                send_one(stage, sb, rb, p, y, z)
            return carry

        lax.fori_loop(low, gx, send, 0)

    def send_above(stage, sb, rb):
        def send(k, carry):
            for y, z in spots:
                send_one(stage, sb, rb, top - k, y, z)
            return carry

        lax.fori_loop(0, top - gx, send, 0)

    def send_plane(stage, sb, rb):
        others(lambda y, z: send_one(stage, sb, rb, gx, y, z))
        pltpu.make_async_copy(sb.at[me], rb.at[me], r_sem).start()

    with scope("i_send0"):
        send_below(0, sb1, rb1)
        send_plane(0, sb1, rb1)
    with scope("j_ready"):
        pl.semaphore_wait(ready, plane - 1)
    with scope("k_send0"):
        if relay:
            start_when(gx == 0, raw_copies)
        send_above(0, sb1, rb1)

    with scope("l_halo"):
        done(edge_rows, h_sem)
        if relay:
            for copy in edge_copies:
                copy.start()

    with scope("m_pack1"):
        line_id = iota((lines, width), 0)
        first_j = line_id % sy == 0
        lane = iota((1, lines), 1)
        at_j0 = lane % sy == 0

        def back_j(x, edge):
            edge_full = jnp.broadcast_to(edge, (sx, sy, width)).reshape(lines, width)
            shifted = jnp.concatenate([x[lines - 1 :, :], x[: lines - 1, :]], axis=0)
            return jnp.where(first_j, edge_full, shifted)

        def neighbours(w, hx, hy, hc):
            edge = hy[...]
            x1 = jnp.concatenate([hx[...], w[: lines - sy, :]], axis=0)
            x2 = back_j(w, edge)
            x3 = back_j(x1, jnp.concatenate([hc[...].reshape(1, 1, width), edge[: sx - 1]], axis=0))
            return x1, x2, x3

        def rim_rows(hr, mine_b, rank, slot):
            r0, rx, ry, rxy = hr[0], hr[1], hr[2], hr[3]
            rim1 = jnp.where(lane < sy, roll_lanes(rx, sy), roll_lanes(r0, sy))
            rim2 = jnp.where(at_j0, roll_lanes(ry, 1 - sy), roll_lanes(r0, 1))
            edge_rim = jnp.where(lane == 0, roll_lanes(rxy, 1), roll_lanes(ry, 1))
            rim3 = jnp.where(at_j0, edge_rim, roll_lanes(rim1, 1))
            rims = slot
            for q, rim in enumerate((r0, rim1, rim2, rim3)):
                rims = jnp.where(group == q, rim, rims)
            rims = jnp.where((rank == row_id % s) & (group < 5), rims, 0.0)
            return pick(mine_b, rims, NT)

        for c, x in enumerate(neighbours(w, hx, hy, hc)):
            sb2[:, c * s : (c + 1) * s, :] = pick(place, x).reshape(n, s, width)
        sb2[:, 3 * s : 3 * s + 1, :] = rim_rows(hr, mine_b, rank, slot).reshape(n, 1, width)

    with scope("n_send1"):
        send_below(1, sb2, rb2)
        send_above(1, sb2, rb2)
        send_plane(1, sb2, rb2)

    def send_theirs():
        end = jnp.where(gx == 1, 0, nx - 1)
        pairs = ((vb1, rb1), (vb2, rb2))

        def to(p, y, z):
            for stage, (sb, rb) in enumerate(pairs):
                pltpu.make_async_remote_copy(
                    src_ref=sb.at[(p - base) * plane + y * nz + z], dst_ref=rb.at[theirs],
                    send_sem=s_sem, recv_sem=r_sem,
                    device_id=(p, y, z), device_id_type=MESH,
                ).start()

        @pl.when(middle)
        def _():
            for y, z in spots:
                to(end, y, z)

        others(lambda y, z: to(gx, y, z))
        for stage, (sb, rb) in enumerate(pairs):
            pltpu.make_async_copy(sb.at[(gx - base) * plane + here], rb.at[theirs], r_sem).start()

    if relay:
        with scope("o_wait0"):
            done(edge_rows + lines // width, v_sem.at[0])
        with scope("o_prep"):
            _, rank_v, goes_v, slot_v = ranks(raw_own[...])
            place_v = onehot(goes_v - base * plane * s == iota((lines // 2, lines), 0))
            mine_v = onehot(raw_own[...] // lines - base * plane == iota((half, lines), 0))
            vb2[:, 3 * s : 3 * s + 1, :] = rim_rows(vr, mine_v, rank_v, slot_v).reshape(half, 1, width)
        with scope("o_wait1"):
            done(lines, v_sem.at[1])
        with scope("o_pack"):
            x0 = raw[...]
            vb1[...] = pick(place_v, x0).reshape(half, s, width)
            for c, x in enumerate(neighbours(x0, vx, vy, vc)):
                vb2[:, c * s : (c + 1) * s, :] = pick(place_v, x).reshape(half, s, width)
        with scope("o_send"):
            send_theirs()

    with scope("q_wait"):
        done(n * pair_rows, r_sem)
    with scope("w_drain"):
        if relay:
            count = 2 * edge_rows + lines + lines // width

            @pl.when(middle)
            def _():
                done(count + (n - plane - 1 + half - 1) * pair_rows, s_sem)

            @pl.when(jnp.logical_not(middle))
            def _():
                done(count + (half - 1 + plane - 1) * pair_rows, s_sem)

        else:
            done(edge_rows + (n - 1) * pair_rows, s_sem)


def finish(n, parts, rb1, rb2, out_hbm, lump_hbm, cur, bef, out_ref, lump_ref, sem):
    lines, width = lump_ref.shape
    s = lines // n
    extra = rb2[:, 3 * s : 3 * s + 1, :]
    spread = jnp.broadcast_to(extra, (n, s, width)).reshape(lines, width)
    spread = jnp.where(iota((lines, width), 1) % s == iota((lines, width), 0) % s, spread, 0.0)
    sums = onehot(iota((8, width), 1) // s == iota((8, width), 0))
    rows = pick(sums, spread, NT)
    slot = rows[4:5, :].astype(I32)
    rims = halves(jnp.concatenate([rows, jnp.zeros((width - 8, lines), F32)], axis=0))
    got = [halves(rb1[...].reshape(lines, width) * 0.015625)]
    got += [halves(rb2[:, c * s : (c + 1) * s, :].reshape(lines, width) * 0.015625) for c in range(3)]

    def triple(c, b):
        return (b, 2.0 * (c + b), c)

    def nine(v):
        by_x0 = triple(v[0], v[1])
        by_x1 = triple(v[2], v[3])
        return [triple(by_x0[o1], by_x1[o1]) for o1 in range(3)]

    def copies(first, count):
        part = pl.ds(first, count)
        return (
            pltpu.make_async_copy(out_ref.at[:, part, :], out_hbm.at[:, part, :], sem),
            pltpu.make_async_copy(lump_ref.at[part, :], lump_hbm.at[part, :], sem),
        )

    first = 0
    for count, piece in parts:
        to_slot = onehot(slot == iota((count, lines), 0) + first)
        for c in range(4):
            hi, lo = got[c]
            cur[c, first : first + count, :] = lax.dot_general(to_slot, hi, NN, preferred_element_type=F32) + lax.dot_general(
                to_slot, lo, NN, preferred_element_type=F32
            )
        hi, lo = rims
        bef[first : first + count, :] = lax.dot_general(to_slot, hi, NT, preferred_element_type=F32) + lax.dot_general(
            to_slot, lo, NT, preferred_element_type=F32
        )
        for start in range(first, first + count, piece):
            span = slice(start, start + piece)
            at_0 = iota((piece, width), 1) == 0
            near, far = [], []
            for c in range(4):
                x = cur[c, span, :]
                near.append(x)
                far.append(jnp.where(at_0, bef[span, c : c + 1] * 0.015625, pltpu.roll(x, 1, axis=1)))
            ahead, back = nine(near), nine(far)
            for o1 in range(3):
                for o2 in range(3):
                    for o3, value in enumerate(triple(ahead[o1][o2], back[o1][o2])):
                        out_ref[9 * o1 + 3 * o2 + o3, span, :] = value
            total = functools.reduce(lambda a, b: a + b, near + far)
            lump_ref[span, :] = 1.0 / (27.0 * total)
            for copy in copies(start, piece):
                copy.start()
        first += count
    for copy in copies(0, lines):
        copy.wait()


def shards(sizes, cell_volume, exponent, owner_row):
    sx, sy, width = cell_volume.shape
    lines = sx * sy
    n = sizes[0] * sizes[1] * sizes[2]
    s = lines // n
    vmem = pl.BlockSpec(memory_space=pltpu.VMEM)
    dma = pltpu.SemaphoreType.DMA
    rb1, rb2 = pl.pallas_call(
        functools.partial(exchange, sizes),
        out_shape=(
            jax.ShapeDtypeStruct((n, s, width), F32),
            jax.ShapeDtypeStruct((n, 3 * s + 1, width), F32),
        ),
        in_specs=[pl.BlockSpec(memory_space=pltpu.HBM)] * 3,
        out_specs=(vmem, vmem),
        scratch_shapes=[
            pltpu.VMEM((sx, sy, width), F32),
            pltpu.VMEM((sx, sy, width), I32),
            pltpu.VMEM((1, lines), I32),
            dma((2,)),
        ]
        + [pltpu.VMEM((n, rows, width), F32) for rows in (s, 3 * s + 1)]
        + [
            pltpu.VMEM((sy, width), F32),
            pltpu.VMEM((sx, 1, width), F32),
            pltpu.VMEM((1, width), F32),
            pltpu.VMEM((1, lines), F32),
            pltpu.VMEM((sy, width), F32),
            pltpu.VMEM((sx, 1, width), F32),
            pltpu.VMEM((1, width), F32),
            pltpu.VMEM((4, 1, lines), F32),
            dma,
            dma,
            dma,
            dma((2,)),
            pltpu.SemaphoreType.REGULAR,
        ]
        + [pltpu.VMEM((n // 2, rows, width), F32) for rows in (s, 3 * s + 1)]
        + [
            pltpu.VMEM((lines, width), F32),
            pltpu.VMEM((lines, width), F32),
            pltpu.VMEM((1, lines), I32),
            pltpu.VMEM((sy, width), F32),
            pltpu.VMEM((sx, 1, width), F32),
            pltpu.VMEM((1, width), F32),
            pltpu.VMEM((4, 1, lines), F32),
            pltpu.VMEM((2 * n * (4 * s + 1), width), F32),
        ],
        compiler_params=pltpu.CompilerParams(
            collective_id=0, has_side_effects=True, vmem_limit_bytes=16 << 20
        ),
    )(*(pltpu.with_memory_space_constraint(a, pltpu.HBM) for a in (cell_volume, exponent, owner_row.reshape(1, lines))))
    parts = [(lines // 4, lines // 8)] * 4
    return pl.pallas_call(
        functools.partial(finish, n, parts),
        out_shape=(
            jax.ShapeDtypeStruct((27, lines, width), F32),
            jax.ShapeDtypeStruct((lines, width), F32),
        ),
        in_specs=[vmem, vmem],
        out_specs=(pl.BlockSpec(memory_space=pltpu.HBM), pl.BlockSpec(memory_space=pltpu.HBM)),
        scratch_shapes=[
            pltpu.VMEM((4, lines, width), F32),
            pltpu.VMEM((lines, width), F32),
            pltpu.VMEM((27, lines, width), F32),
            pltpu.VMEM((lines, width), F32),
            dma,
        ],
        compiler_params=pltpu.CompilerParams(vmem_limit_bytes=16 << 20),
    )(rb1, rb2)


def solution(mesh):
    sizes = tuple(mesh.shape[a] for a in AXES)
    return jax.shard_map(
        functools.partial(shards, sizes),
        mesh=mesh,
        in_specs=(P(*AXES), P(*AXES), P(AXES)),
        out_specs=(P(None, AXES, None), P(AXES, None)),
        check_vma=False,
    )
```

```python
import functools

import jax
import jax.numpy as jnp
from jax import lax
from jax.experimental import pallas as pl
from jax.experimental.pallas import tpu as pltpu
from jax.sharding import PartitionSpec as P

MESH = pl.DeviceIdType.MESH
AXES = ("gx", "gy", "gz")
F32, BF16, I32 = jnp.float32, jnp.bfloat16, jnp.int32
log_step = 0.3
NN = (((1,), (0,)), ((), ()))
NT = (((1,), (1,)), ((), ()))


def onehot(mask):
    return jnp.where(mask, 1.0, 0.0).astype(BF16)


def halves(x):
    hi = x.astype(BF16)
    return hi, (x - hi.astype(F32)).astype(BF16)


def pick(sel, x, dims=NN):
    total = None
    for part in halves(x):
        term = lax.dot_general(sel, part, dims, preferred_element_type=F32)
        total = term if total is None else total + term
    return total


def pick_r(x, sel, dims=NN):
    total = None
    for part in halves(x):
        term = lax.dot_general(part, sel, dims, preferred_element_type=F32)
        total = term if total is None else total + term
    return total


def iota(shape, dim):
    return lax.broadcasted_iota(I32, shape, dim)


def roll_lanes(x, shift):
    width = x.shape[1]
    cut = width - shift % width
    return jnp.concatenate([x[:, cut:], x[:, :cut]], axis=1)


def exchange(
    sizes, cv_hbm, ex_hbm, own_hbm, rb,
    cv_ref, ex_ref, own_ref, in_sem,
    sb, tx, ty, tc, tr, hx, hy, hc, hr,
    s_sem, r_sem, h_sem, v_sem, ready, above,
    vb, wv, raw, raw_own, vx, vy, vc, vr, tally,
):
    nx, ny, nz = sizes
    plane = ny * nz
    n = nx * plane
    gx, gy, gz = (lax.axis_index(a) for a in AXES)
    here = gy * nz + gz
    me = gx * plane + here
    sx, sy, width = cv_ref.shape
    lines = sx * sy
    s = lines // n
    relay = nx == 4
    half = n // 2
    base = (gx // 2) * 2
    middle = (gx == 1) | (gx == 2)
    across, beside = (gx + 2) % nx, jnp.where(gx < 2, 1 - gx, nx + 1 - gx)
    give, take = jnp.where(middle, beside, across), jnp.where(middle, across, beside)
    theirs = take * plane + here
    spots = [(y, z) for y in range(ny) for z in range(nz)]
    ux, uy, uz = (gx + 1) % nx, (gy + 1) % ny, (gz + 1) % nz
    dx, dy, dz = (gx + nx - 1) % nx, (gy + ny - 1) % ny, (gz + nz - 1) % nz

    def signal(sem, to):
        pl.semaphore_signal(sem, inc=1, device_id=to, device_id_type=MESH)

    def others(visit):
        for y in range(ny):
            for z in range(nz):
                if y or z:
                    visit((gy + y) % ny, (gz + z) % nz)

    def done(rows, sem):
        part = tally.at[pl.ds(0, rows)]
        pltpu.make_async_copy(part, part, sem).wait()

    edge_rows = sx + sy + 1 + 4 * lines // width
    pair_rows = 4 * s + 1

    scope = jax.named_scope
    with scope("a_in"):
        arrive = []
        for i, (src, dst) in enumerate(((own_hbm, own_ref), (cv_hbm, cv_ref), (ex_hbm, ex_ref))):
            copy = pltpu.make_async_copy(src, dst, in_sem.at[min(i, 1)])
            copy.start()
            arrive.append(copy)
    with scope("b_bar"):
        barrier = pltpu.get_barrier_semaphore()
        others(lambda y, z: signal(barrier, (gx, y, z)))
        corners = [(dy, gz), (gy, dz), (dy, dz)]

        @pl.when(gx > 0)
        def _():
            for y, z in corners:
                signal(barrier, (dx, y, z))

        def greet_below(p, carry):
            signal(barrier, (p, gy, gz))
            return carry

        reach = 1 if relay else nx
        lax.fori_loop(jnp.maximum(gx - reach, 0), gx, greet_below, 0)

        def greet_above(p, carry):
            if relay:

                @pl.when(p == 1)
                def _():
                    signal(barrier, (p, gy, gz))

                @pl.when(p > 1)
                def _():
                    for y, z in spots:
                        signal(barrier, (p, y, z))
            else:
                for y, z in spots:
                    signal(barrier, (p, y, z))
            return carry

        lax.fori_loop(gx + 1, nx, greet_above, 0)
        expect = plane - 1 + gx * plane + jnp.minimum(nx - 1 - gx, reach) + jnp.where(gx < nx - 1, len(corners), 0)
        if relay:
            expect -= jnp.where(gx == 1, plane - 1, 0)

    with scope("c_own"):
        arrive[0].wait()
        def ranks(own):
            owner = own // lines
            mine = owner == iota((n, lines), 0)
            counts = lax.dot_general(onehot(mine), below, NN, preferred_element_type=F32)
            rank = jnp.sum(jnp.where(mine, counts, 0.0), axis=0, keepdims=True).astype(I32)
            return onehot(mine), rank, owner * s + rank, (own % lines).astype(F32)

        below = onehot(iota((lines, lines), 0) < iota((lines, lines), 1))
        mine_b, rank, goes, slot = ranks(own_ref[...])
        place = onehot(goes == iota((lines, lines), 0))
        row_id = iota((width, lines), 0)
        group = row_id // s

    with scope("d_inwait"):
        done(2 * lines, in_sem.at[1])
    with scope("e_pack0"):
        w3 = cv_ref[...] * jnp.exp(-log_step * ex_ref[...].astype(F32))
        w = w3.reshape(lines, width)
        wv[...] = w
        tx[...] = w[lines - sy :, :]
        ty[...] = w3[:, sy - 1 :, :]
        tc[...] = w[lines - 1 :, :]
        last = onehot(iota((8, width), 1) == width - 1)
        tr[...] = pick(last, w, NT)[0:1, :]
        sb[:, 0:s, :] = pick(place, w).reshape(n, s, width)

    with scope("g_barwait"):
        pl.semaphore_wait(barrier, expect)
        others(lambda y, z: signal(ready, (gx, y, z)))
        if relay:

            @pl.when(gx == 1)
            def _():
                signal(above, (0, gy, gz))


    with scope("h_halosend"):
        routes = [
            (tx, hx, (ux, gy, gz)),
            (ty, hy, (gx, uy, gz)),
            (tc, hc, (ux, uy, gz)),
            (tr, hr.at[0], (gx, gy, uz)),
            (tr, hr.at[1], (ux, gy, uz)),
            (tr, hr.at[2], (gx, uy, uz)),
            (tr, hr.at[3], (ux, uy, uz)),
        ]
        for i, (src, dst, to) in enumerate(routes):
            copy = pltpu.make_async_remote_copy(
                src_ref=src, dst_ref=dst, send_sem=s_sem, recv_sem=h_sem.at[0 if src is ty else 1],
                device_id=to, device_id_type=MESH,
            )
            copy.start()

    def hand(sem, src, dst, to):
        return pltpu.make_async_remote_copy(
            src_ref=src, dst_ref=dst, send_sem=s_sem, recv_sem=sem, device_id=to, device_id_type=MESH
        )

    raw_copies = [hand(v_sem.at[2], own_ref, raw_own, (give, gy, gz)), hand(v_sem.at[1], wv, raw, (give, gy, gz))]
    back = jnp.maximum(gx - 1, 0)
    back_copies = [
        hand(v_sem.at[0], tx, vx, (back, gy, gz)),
        hand(v_sem.at[0], tc, vc, (back, uy, gz)),
        hand(v_sem.at[0], tr, vr.at[1], (back, gy, uz)),
        hand(v_sem.at[0], tr, vr.at[3], (back, uy, uz)),
    ]
    side_copies = [
        hand(v_sem.at[0], ty, vy, (across, uy, gz)),
        hand(v_sem.at[0], tr, vr.at[0], (across, gy, uz)),
        hand(v_sem.at[0], tr, vr.at[2], (across, uy, uz)),
    ]
    edge_copies = [
        hand(v_sem.at[0], src, dst, (give, gy, gz)) for src, dst in ((hx, vx), (hy, vy), (hc, vc), (hr, vr))
    ]

    def start_when(flag, copies):
        @pl.when(flag)
        def _():
            for copy in copies:
                copy.start()

    if relay:
        with scope("h_raw"):
            start_when(gx >= 2, back_copies)
            start_when(gx == nx - 1, side_copies)
            start_when(gx > 0, raw_copies)

    def send_one(p, y, z):
        pltpu.make_async_remote_copy(
            src_ref=sb.at[p * plane + y * nz + z], dst_ref=rb.at[me], send_sem=s_sem, recv_sem=r_sem,
            device_id=(p, y, z), device_id_type=MESH,
        ).start()

    low, top = 0, nx - 1
    if relay:
        low = jnp.where(gx == 2, 0, jnp.where(gx == 1, 1, base))
        top = jnp.where(gx == 1, nx - 1, jnp.where(gx == 2, 2, base + 1))

    def send_below():
        def send(p, carry):
            for y, z in spots:
                send_one(p, y, z)
            return carry

        lax.fori_loop(low, gx, send, 0)

    def send_above():
        def send(k, carry):
            for y, z in spots:
                send_one(top - k, y, z)
            return carry

        lax.fori_loop(0, top - gx, send, 0)

    def send_plane(first, count):
        def to(y, z):
            d = gx * plane + y * nz + z
            part = pl.ds(first, count)
            pltpu.make_async_remote_copy(
                src_ref=sb.at[d, part], dst_ref=rb.at[me, part], send_sem=s_sem, recv_sem=r_sem,
                device_id=(gx, y, z), device_id_type=MESH,
            ).start()

        others(to)

    split = 2 * s if (2 * s) % 8 == 0 else 0

    with scope("j_ready"):
        pl.semaphore_wait(ready, plane - 1)
    with scope("k_send0"):
        if relay:

            @pl.when(gx == 2)
            def _():
                signal(above, (1, gy, gz))

            @pl.when(gx == 0)
            def _():
                pl.semaphore_wait(above, 1)

            start_when(gx == 0, side_copies + raw_copies)

    line_id = iota((lines, width), 0)
    first_j = line_id % sy == 0
    lane = iota((1, lines), 1)
    at_j0 = lane % sy == 0

    def back_j(x, edge):
        edge_full = jnp.broadcast_to(edge, (sx, sy, width)).reshape(lines, width)
        shifted = jnp.concatenate([x[lines - 1 :, :], x[: lines - 1, :]], axis=0)
        return jnp.where(first_j, edge_full, shifted)

    def behind_i(w, hx, hy, hc):
        x1 = jnp.concatenate([hx[...], w[: lines - sy, :]], axis=0)
        return x1, back_j(x1, jnp.concatenate([hc[...].reshape(1, 1, width), hy[...][: sx - 1]], axis=0))

    def rim_rows(hr, mine_b, rank, slot):
        r0, rx, ry, rxy = hr[0], hr[1], hr[2], hr[3]
        rim1 = jnp.where(lane < sy, roll_lanes(rx, sy), roll_lanes(r0, sy))
        rim2 = jnp.where(at_j0, roll_lanes(ry, 1 - sy), roll_lanes(r0, 1))
        edge_rim = jnp.where(lane == 0, roll_lanes(rxy, 1), roll_lanes(ry, 1))
        rim3 = jnp.where(at_j0, edge_rim, roll_lanes(rim1, 1))
        rims = slot
        for q, rim in enumerate((r0, rim1, rim2, rim3)):
            rims = jnp.where(group == q, rim, rims)
        rims = jnp.where((rank == row_id % s) & (group < 5), rims, 0.0)
        return pick(mine_b, rims, NT)

    with scope("l_halo0"):
        done(sx, h_sem.at[0])
    with scope("l_pack"):
        sb[:, s : 2 * s, :] = pick(place, back_j(w, hy[...])).reshape(n, s, width)
        if split:
            send_plane(0, split)
    with scope("l_halo1"):
        done(edge_rows - sx, h_sem.at[1])
        if relay:
            start_when(middle, edge_copies)
    with scope("m_pack1"):
        for c, x in enumerate(behind_i(w, hx, hy, hc)):
            sb[:, (c + 2) * s : (c + 3) * s, :] = pick(place, x).reshape(n, s, width)
        sb[:, 4 * s : 4 * s + 1, :] = rim_rows(hr, mine_b, rank, slot).reshape(n, 1, width)

    with scope("n_send1"):
        send_below()
        if relay:

            @pl.when(gx == 1)
            def _():
                pl.semaphore_wait(above, 1)

        send_above()
        send_plane(split, pair_rows - split)
        pltpu.make_async_copy(sb.at[me], rb.at[me], r_sem).start()

    def send_theirs():
        end = jnp.where(gx == 1, 0, nx - 1)

        def to(p, y, z):
            pltpu.make_async_remote_copy(
                src_ref=vb.at[(p - base) * plane + y * nz + z], dst_ref=rb.at[theirs], send_sem=s_sem, recv_sem=r_sem,
                device_id=(p, y, z), device_id_type=MESH,
            ).start()

        @pl.when(middle)
        def _():
            for y, z in spots:
                to(end, y, z)

        others(lambda y, z: to(gx, y, z))
        pltpu.make_async_copy(vb.at[(gx - base) * plane + here], rb.at[theirs], r_sem).start()

    if relay:
        with scope("o_prep"):
            done(lines // width, v_sem.at[2])
            _, rank_v, goes_v, slot_v = ranks(raw_own[...])
            place_v = onehot(goes_v - base * plane * s == iota((lines // 2, lines), 0))
            mine_v = onehot(raw_own[...] // lines - base * plane == iota((half, lines), 0))
        with scope("o_wait0"):
            done(edge_rows, v_sem.at[0])
        with scope("o_rim"):
            vb[:, 4 * s : 4 * s + 1, :] = rim_rows(vr, mine_v, rank_v, slot_v).reshape(half, 1, width)
        with scope("o_wait1"):
            done(lines, v_sem.at[1])
        with scope("o_pack"):
            x0 = raw[...]
            for c, x in enumerate((x0, back_j(x0, vy[...]), *behind_i(x0, vx, vy, vc))):
                vb[:, c * s : (c + 1) * s, :] = pick(place_v, x).reshape(half, s, width)
        with scope("o_send"):
            send_theirs()

    with scope("q_wait"):
        done(n * pair_rows, r_sem)
    with scope("w_drain"):
        if relay:
            count = edge_rows + lines + lines // width
            back_rows = sy + 1 + 2 * lines // width

            @pl.when(gx >= 2)
            def _():
                done(back_rows, s_sem)


            @pl.when(middle)
            def _():
                done(count + edge_rows + (n - plane - 1 + half - 1) * pair_rows, s_sem)

            @pl.when(jnp.logical_not(middle))
            def _():
                done(count + edge_rows - back_rows + (half - 1 + plane - 1) * pair_rows, s_sem)

        else:
            done(edge_rows + (n - 1) * pair_rows, s_sem)


def finish(n, parts, rb, out_hbm, lump_hbm, cur, bef, out_ref, lump_ref, sem):
    lines, width = lump_ref.shape
    s = lines // n
    extra = rb[:, 4 * s : 4 * s + 1, :]
    spread = jnp.broadcast_to(extra, (n, s, width)).reshape(lines, width)
    spread = jnp.where(iota((lines, width), 1) % s == iota((lines, width), 0) % s, spread, 0.0)
    sums = onehot(iota((8, width), 1) // s == iota((8, width), 0))
    rows = pick(sums, spread, NT)
    slot = rows[4:5, :].astype(I32)
    rims = halves(jnp.concatenate([rows, jnp.zeros((width - 8, lines), F32)], axis=0))
    got = [halves(rb[:, c * s : (c + 1) * s, :].reshape(lines, width) * 0.015625) for c in (0, 2, 1, 3)]

    def triple(c, b):
        return (b, 2.0 * (c + b), c)

    def nine(v):
        by_x0 = triple(v[0], v[1])
        by_x1 = triple(v[2], v[3])
        return [triple(by_x0[o1], by_x1[o1]) for o1 in range(3)]

    def copies(first, count):
        part = pl.ds(first, count)
        return (
            pltpu.make_async_copy(out_ref.at[:, part, :], out_hbm.at[:, part, :], sem),
            pltpu.make_async_copy(lump_ref.at[part, :], lump_hbm.at[part, :], sem),
        )

    first = 0
    for count, piece in parts:
        to_slot = onehot(slot == iota((count, lines), 0) + first)
        for c in range(4):
            hi, lo = got[c]
            cur[c, first : first + count, :] = lax.dot_general(to_slot, hi, NN, preferred_element_type=F32) + lax.dot_general(
                to_slot, lo, NN, preferred_element_type=F32
            )
        hi, lo = rims
        bef[first : first + count, :] = lax.dot_general(to_slot, hi, NT, preferred_element_type=F32) + lax.dot_general(
            to_slot, lo, NT, preferred_element_type=F32
        )
        for start in range(first, first + count, piece):
            span = slice(start, start + piece)
            at_0 = iota((piece, width), 1) == 0
            near, far = [], []
            for c in range(4):
                x = cur[c, span, :]
                near.append(x)
                far.append(jnp.where(at_0, bef[span, c : c + 1] * 0.015625, pltpu.roll(x, 1, axis=1)))
            ahead, back = nine(near), nine(far)
            for o1 in range(3):
                for o2 in range(3):
                    for o3, value in enumerate(triple(ahead[o1][o2], back[o1][o2])):
                        out_ref[9 * o1 + 3 * o2 + o3, span, :] = value
            total = functools.reduce(lambda a, b: a + b, near + far)
            lump_ref[span, :] = 1.0 / (27.0 * total)
            for copy in copies(start, piece):
                copy.start()
        first += count
    for copy in copies(0, lines):
        copy.wait()


def shards(sizes, cell_volume, exponent, owner_row):
    sx, sy, width = cell_volume.shape
    lines = sx * sy
    n = sizes[0] * sizes[1] * sizes[2]
    s = lines // n
    vmem = pl.BlockSpec(memory_space=pltpu.VMEM)
    dma = pltpu.SemaphoreType.DMA
    received = pl.pallas_call(
        functools.partial(exchange, sizes),
        out_shape=jax.ShapeDtypeStruct((n, 4 * s + 1, width), F32),
        in_specs=[pl.BlockSpec(memory_space=pltpu.HBM)] * 3,
        out_specs=vmem,
        scratch_shapes=[
            pltpu.VMEM((sx, sy, width), F32),
            pltpu.VMEM((sx, sy, width), I32),
            pltpu.VMEM((1, lines), I32),
            dma((2,)),
        ]
        + [
            pltpu.VMEM((n, 4 * s + 1, width), F32),
            pltpu.VMEM((sy, width), F32),
            pltpu.VMEM((sx, 1, width), F32),
            pltpu.VMEM((1, width), F32),
            pltpu.VMEM((1, lines), F32),
            pltpu.VMEM((sy, width), F32),
            pltpu.VMEM((sx, 1, width), F32),
            pltpu.VMEM((1, width), F32),
            pltpu.VMEM((4, 1, lines), F32),
            dma,
            dma,
            dma((2,)),
            dma((3,)),
            pltpu.SemaphoreType.REGULAR,
            pltpu.SemaphoreType.REGULAR,
        ]
        + [
            pltpu.VMEM((n // 2, 4 * s + 1, width), F32),
            pltpu.VMEM((lines, width), F32),
            pltpu.VMEM((lines, width), F32),
            pltpu.VMEM((1, lines), I32),
            pltpu.VMEM((sy, width), F32),
            pltpu.VMEM((sx, 1, width), F32),
            pltpu.VMEM((1, width), F32),
            pltpu.VMEM((4, 1, lines), F32),
            pltpu.VMEM((2 * n * (4 * s + 1), width), F32),
        ],
        compiler_params=pltpu.CompilerParams(
            collective_id=0, has_side_effects=True, vmem_limit_bytes=16 << 20
        ),
    )(*(pltpu.with_memory_space_constraint(a, pltpu.HBM) for a in (cell_volume, exponent, owner_row.reshape(1, lines))))
    parts = [(lines // 4, lines // 8)] * 4
    return pl.pallas_call(
        functools.partial(finish, n, parts),
        out_shape=(
            jax.ShapeDtypeStruct((27, lines, width), F32),
            jax.ShapeDtypeStruct((lines, width), F32),
        ),
        in_specs=[vmem],
        out_specs=(pl.BlockSpec(memory_space=pltpu.HBM), pl.BlockSpec(memory_space=pltpu.HBM)),
        scratch_shapes=[
            pltpu.VMEM((4, lines, width), F32),
            pltpu.VMEM((lines, width), F32),
            pltpu.VMEM((27, lines, width), F32),
            pltpu.VMEM((lines, width), F32),
            dma,
        ],
        compiler_params=pltpu.CompilerParams(vmem_limit_bytes=16 << 20),
    )(received)


def solution(mesh):
    sizes = tuple(mesh.shape[a] for a in AXES)
    return jax.shard_map(
        functools.partial(shards, sizes),
        mesh=mesh,
        in_specs=(P(*AXES), P(*AXES), P(AXES)),
        out_specs=(P(None, AXES, None), P(AXES, None)),
        check_vma=False,
    )
```

```python
import functools

import jax
import jax.numpy as jnp
from jax import lax
from jax.experimental import pallas as pl
from jax.experimental.pallas import tpu as pltpu
from jax.sharding import PartitionSpec as P

MESH = pl.DeviceIdType.MESH
AXES = ("gx", "gy", "gz")
F32, BF16, I32 = jnp.float32, jnp.bfloat16, jnp.int32
log_step = 0.3
NN = (((1,), (0,)), ((), ()))
NT = (((1,), (1,)), ((), ()))


def onehot(mask):
    return jnp.where(mask, 1.0, 0.0).astype(BF16)


def halves(x):
    hi = x.astype(BF16)
    return hi, (x - hi.astype(F32)).astype(BF16)


def pick(sel, x, dims=NN):
    total = None
    for part in halves(x):
        term = lax.dot_general(sel, part, dims, preferred_element_type=F32)
        total = term if total is None else total + term
    return total


def pick_r(x, sel, dims=NN):
    total = None
    for part in halves(x):
        term = lax.dot_general(part, sel, dims, preferred_element_type=F32)
        total = term if total is None else total + term
    return total


def iota(shape, dim):
    return lax.broadcasted_iota(I32, shape, dim)


def roll_lanes(x, shift):
    width = x.shape[1]
    cut = width - shift % width
    return jnp.concatenate([x[:, cut:], x[:, :cut]], axis=1)


def exchange(
    sizes, cv_hbm, ex_hbm, own_hbm, rb,
    cv_ref, ex_ref, own_ref, in_sem,
    sb, tx, ty, tc, tr, hx, hy, hc, hr,
    s_sem, r_sem, h_sem, v_sem, ready, above,
    vb, wv, raw, raw_own, vx, vy, vc, vr, tally,
):
    nx, ny, nz = sizes
    plane = ny * nz
    n = nx * plane
    gx, gy, gz = (lax.axis_index(a) for a in AXES)
    here = gy * nz + gz
    me = gx * plane + here
    sx, sy, width = cv_ref.shape
    lines = sx * sy
    s = lines // n
    relay = nx == 4
    half = n // 2
    base = (gx // 2) * 2
    middle = (gx == 1) | (gx == 2)
    across, beside = (gx + 2) % nx, jnp.where(gx < 2, 1 - gx, nx + 1 - gx)
    give, take = jnp.where(middle, beside, across), jnp.where(middle, across, beside)
    theirs = take * plane + here
    spots = [(y, z) for y in range(ny) for z in range(nz)]
    ux, uy, uz = (gx + 1) % nx, (gy + 1) % ny, (gz + 1) % nz
    dx, dy, dz = (gx + nx - 1) % nx, (gy + ny - 1) % ny, (gz + nz - 1) % nz

    def signal(sem, to):
        pl.semaphore_signal(sem, inc=1, device_id=to, device_id_type=MESH)

    def others(visit):
        for y in range(ny):
            for z in range(nz):
                if y or z:
                    visit((gy + y) % ny, (gz + z) % nz)

    def done(rows, sem):
        part = tally.at[pl.ds(0, rows)]
        pltpu.make_async_copy(part, part, sem).wait()

    edge_rows = sx + sy + 1 + 4 * lines // width
    pair_rows = 4 * s + 1

    scope = jax.named_scope
    with scope("a_in"):
        arrive = []
        for i, (src, dst) in enumerate(((own_hbm, own_ref), (cv_hbm, cv_ref), (ex_hbm, ex_ref))):
            copy = pltpu.make_async_copy(src, dst, in_sem.at[min(i, 1)])
            copy.start()
            arrive.append(copy)
    with scope("b_bar"):
        barrier = pltpu.get_barrier_semaphore()
        others(lambda y, z: signal(barrier, (gx, y, z)))
        corners = [(dy, gz), (gy, dz), (dy, dz)]

        @pl.when(gx > 0)
        def _():
            for y, z in corners:
                signal(barrier, (dx, y, z))

        def greet_below(p, carry):
            signal(barrier, (p, gy, gz))
            return carry

        reach = 1 if relay else nx
        lax.fori_loop(jnp.maximum(gx - reach, 0), gx, greet_below, 0)

        def greet_above(p, carry):
            if relay:

                @pl.when(p == 1)
                def _():
                    signal(barrier, (p, gy, gz))

                @pl.when(p > 1)
                def _():
                    for y, z in spots:
                        signal(barrier, (p, y, z))
            else:
                for y, z in spots:
                    signal(barrier, (p, y, z))
            return carry

        lax.fori_loop(gx + 1, nx, greet_above, 0)
        expect = plane - 1 + gx * plane + jnp.minimum(nx - 1 - gx, reach) + jnp.where(gx < nx - 1, len(corners), 0)
        if relay:
            expect -= jnp.where(gx == 1, plane - 1, 0)

    with scope("c_own"):
        arrive[0].wait()
        def ranks(own):
            owner = own // lines
            mine = owner == iota((n, lines), 0)
            counts = lax.dot_general(onehot(mine), below, NN, preferred_element_type=F32)
            rank = jnp.sum(jnp.where(mine, counts, 0.0), axis=0, keepdims=True).astype(I32)
            return onehot(mine), rank, owner * s + rank, (own % lines).astype(F32)

        below = onehot(iota((lines, lines), 0) < iota((lines, lines), 1))
        mine_b, rank, goes, slot = ranks(own_ref[...])
        place = onehot(goes == iota((lines, lines), 0))
        row_id = iota((width, lines), 0)
        group = row_id // s

    with scope("d_inwait"):
        done(2 * lines, in_sem.at[1])
    with scope("e_pack0"):
        w3 = cv_ref[...] * jnp.exp(-log_step * ex_ref[...].astype(F32))
        w = w3.reshape(lines, width)
        wv[...] = w
        tx[...] = w[lines - sy :, :]
        ty[...] = w3[:, sy - 1 :, :]
        tc[...] = w[lines - 1 :, :]
        last = onehot(iota((8, width), 1) == width - 1)
        tr[...] = pick(last, w, NT)[0:1, :]
        sb[:, 0:s, :] = pick(place, w).reshape(n, s, width)

    with scope("g_barwait"):
        pl.semaphore_wait(barrier, expect)
        others(lambda y, z: signal(ready, (gx, y, z)))
        if relay:

            @pl.when(gx == 1)
            def _():
                signal(above, (0, gy, gz))


    with scope("h_halosend"):
        routes = [
            (tx, hx, (ux, gy, gz)),
            (ty, hy, (gx, uy, gz)),
            (tc, hc, (ux, uy, gz)),
            (tr, hr.at[0], (gx, gy, uz)),
            (tr, hr.at[1], (ux, gy, uz)),
            (tr, hr.at[2], (gx, uy, uz)),
            (tr, hr.at[3], (ux, uy, uz)),
        ]
        for i, (src, dst, to) in enumerate(routes):
            copy = pltpu.make_async_remote_copy(
                src_ref=src, dst_ref=dst, send_sem=s_sem, recv_sem=h_sem.at[0 if src is ty else 1],
                device_id=to, device_id_type=MESH,
            )
            copy.start()

    def hand(sem, src, dst, to):
        return pltpu.make_async_remote_copy(
            src_ref=src, dst_ref=dst, send_sem=s_sem, recv_sem=sem, device_id=to, device_id_type=MESH
        )

    raw_copies = [hand(v_sem.at[2], own_ref, raw_own, (give, gy, gz)), hand(v_sem.at[1], wv, raw, (give, gy, gz))]
    back = jnp.maximum(gx - 1, 0)
    back_copies = [
        hand(v_sem.at[0], tx, vx, (back, gy, gz)),
        hand(v_sem.at[0], tc, vc, (back, uy, gz)),
        hand(v_sem.at[0], tr, vr.at[1], (back, gy, uz)),
        hand(v_sem.at[0], tr, vr.at[3], (back, uy, uz)),
    ]
    side_copies = [
        hand(v_sem.at[0], ty, vy, (across, uy, gz)),
        hand(v_sem.at[0], tr, vr.at[0], (across, gy, uz)),
        hand(v_sem.at[0], tr, vr.at[2], (across, uy, uz)),
    ]
    edge_copies = [
        hand(v_sem.at[0], src, dst, (give, gy, gz)) for src, dst in ((hx, vx), (hy, vy), (hc, vc), (hr, vr))
    ]

    def part_to(p, y, z, first, count):
        d, part = p * plane + y * nz + z, pl.ds(first, count)
        pltpu.make_async_remote_copy(
            src_ref=sb.at[d, part], dst_ref=rb.at[me, part], send_sem=s_sem, recv_sem=r_sem,
            device_id=(p, y, z), device_id_type=MESH,
        ).start()

    early = s if relay and s % 8 == 0 else 0

    def start_when(flag, copies):
        @pl.when(flag)
        def _():
            for copy in copies:
                copy.start()

    if relay:
        with scope("h_raw"):
            start_when(gx >= 2, back_copies)
            start_when(gx == nx - 1, side_copies)
            start_when(gx > 0, raw_copies)
            if early:

                @pl.when(gx == 2)
                def _():
                    for y, z in spots:
                        part_to(0, y, z, 0, early)


    def send_one(p, y, z):
        pltpu.make_async_remote_copy(
            src_ref=sb.at[p * plane + y * nz + z], dst_ref=rb.at[me], send_sem=s_sem, recv_sem=r_sem,
            device_id=(p, y, z), device_id_type=MESH,
        ).start()

    low, top = 0, nx - 1
    if relay:
        low = jnp.where(gx == 2, 0, jnp.where(gx == 1, 1, base))
        top = jnp.where(gx == 1, nx - 1, jnp.where(gx == 2, 2, base + 1))

    def send_below():
        def send(p, carry):
            for y, z in spots:
                send_one(p, y, z)
            return carry

        if relay:

            @pl.when(gx == 2)
            def _():
                for y, z in spots:
                    part_to(0, y, z, early, pair_rows - early)

        lax.fori_loop(jnp.maximum(low, 1) if relay else 0, gx, send, 0)

    def send_above():
        def send(k, carry):
            for y, z in spots:
                send_one(top - k, y, z)
            return carry

        lax.fori_loop(0, top - gx, send, 0)

    def send_plane(first, count):
        others(lambda y, z: part_to(gx, y, z, first, count))

    split = 2 * s if (2 * s) % 8 == 0 else 0

    with scope("j_ready"):
        pl.semaphore_wait(ready, plane - 1)
    with scope("k_send0"):
        if relay:

            @pl.when(gx == 2)
            def _():
                signal(above, (1, gy, gz))

            @pl.when(gx == 0)
            def _():
                pl.semaphore_wait(above, 1)

            start_when(gx == 0, side_copies + raw_copies)

    line_id = iota((lines, width), 0)
    first_j = line_id % sy == 0
    lane = iota((1, lines), 1)
    at_j0 = lane % sy == 0

    def back_j(x, edge):
        edge_full = jnp.broadcast_to(edge, (sx, sy, width)).reshape(lines, width)
        shifted = jnp.concatenate([x[lines - 1 :, :], x[: lines - 1, :]], axis=0)
        return jnp.where(first_j, edge_full, shifted)

    def behind_i(w, hx, hy, hc):
        x1 = jnp.concatenate([hx[...], w[: lines - sy, :]], axis=0)
        return x1, back_j(x1, jnp.concatenate([hc[...].reshape(1, 1, width), hy[...][: sx - 1]], axis=0))

    def rim_rows(hr, mine_b, rank, slot):
        r0, rx, ry, rxy = hr[0], hr[1], hr[2], hr[3]
        rim1 = jnp.where(lane < sy, roll_lanes(rx, sy), roll_lanes(r0, sy))
        rim2 = jnp.where(at_j0, roll_lanes(ry, 1 - sy), roll_lanes(r0, 1))
        edge_rim = jnp.where(lane == 0, roll_lanes(rxy, 1), roll_lanes(ry, 1))
        rim3 = jnp.where(at_j0, edge_rim, roll_lanes(rim1, 1))
        rims = slot
        for q, rim in enumerate((r0, rim1, rim2, rim3)):
            rims = jnp.where(group == q, rim, rims)
        rims = jnp.where((rank == row_id % s) & (group < 5), rims, 0.0)
        return pick(mine_b, rims, NT)

    with scope("l_halo0"):
        done(sx, h_sem.at[0])
    with scope("l_pack"):
        sb[:, s : 2 * s, :] = pick(place, back_j(w, hy[...])).reshape(n, s, width)
        if split:
            send_plane(0, split)
    with scope("l_halo1"):
        done(edge_rows - sx, h_sem.at[1])
        if relay:
            start_when(middle, edge_copies)
    with scope("m_pack1"):
        for c, x in enumerate(behind_i(w, hx, hy, hc)):
            sb[:, (c + 2) * s : (c + 3) * s, :] = pick(place, x).reshape(n, s, width)
        sb[:, 4 * s : 4 * s + 1, :] = rim_rows(hr, mine_b, rank, slot).reshape(n, 1, width)

    with scope("n_send1"):
        send_below()
        send_plane(split, pair_rows - split)
        pltpu.make_async_copy(sb.at[me], rb.at[me], r_sem).start()
        if relay:

            @pl.when(gx == 1)
            def _():
                pl.semaphore_wait(above, 1)

        send_above()

    def send_theirs():
        end = jnp.where(gx == 1, 0, nx - 1)

        def to(p, y, z):
            pltpu.make_async_remote_copy(
                src_ref=vb.at[(p - base) * plane + y * nz + z], dst_ref=rb.at[theirs], send_sem=s_sem, recv_sem=r_sem,
                device_id=(p, y, z), device_id_type=MESH,
            ).start()

        @pl.when(middle)
        def _():
            for y, z in spots:
                to(end, y, z)

        others(lambda y, z: to(gx, y, z))
        pltpu.make_async_copy(vb.at[(gx - base) * plane + here], rb.at[theirs], r_sem).start()

    if relay:
        with scope("o_prep"):
            done(lines // width, v_sem.at[2])
            _, rank_v, goes_v, slot_v = ranks(raw_own[...])
            place_v = onehot(goes_v - base * plane * s == iota((lines // 2, lines), 0))
            mine_v = onehot(raw_own[...] // lines - base * plane == iota((half, lines), 0))
        with scope("o_wait0"):
            done(edge_rows, v_sem.at[0])
        with scope("o_rim"):
            vb[:, 4 * s : 4 * s + 1, :] = rim_rows(vr, mine_v, rank_v, slot_v).reshape(half, 1, width)
        with scope("o_wait1"):
            done(lines, v_sem.at[1])
        with scope("o_pack"):
            x0 = raw[...]
            for c, x in enumerate((x0, back_j(x0, vy[...]), *behind_i(x0, vx, vy, vc))):
                vb[:, c * s : (c + 1) * s, :] = pick(place_v, x).reshape(half, s, width)
        with scope("o_send"):
            send_theirs()

    with scope("q_wait"):
        done(n * pair_rows, r_sem)
    with scope("w_drain"):
        if relay:
            count = edge_rows + lines + lines // width
            back_rows = sy + 1 + 2 * lines // width

            @pl.when(gx >= 2)
            def _():
                done(back_rows, s_sem)


            @pl.when(middle)
            def _():
                done(count + edge_rows + (n - plane - 1 + half - 1) * pair_rows, s_sem)

            @pl.when(jnp.logical_not(middle))
            def _():
                done(count + edge_rows - back_rows + (half - 1 + plane - 1) * pair_rows, s_sem)

        else:
            done(edge_rows + (n - 1) * pair_rows, s_sem)


def finish(n, parts, rb, out_hbm, lump_hbm, cur, bef, out_ref, lump_ref, sem):
    lines, width = lump_ref.shape
    s = lines // n
    extra = rb[:, 4 * s : 4 * s + 1, :]
    spread = jnp.broadcast_to(extra, (n, s, width)).reshape(lines, width)
    spread = jnp.where(iota((lines, width), 1) % s == iota((lines, width), 0) % s, spread, 0.0)
    sums = onehot(iota((8, width), 1) // s == iota((8, width), 0))
    rows = pick(sums, spread, NT)
    slot = rows[4:5, :].astype(I32)
    rims = halves(jnp.concatenate([rows, jnp.zeros((width - 8, lines), F32)], axis=0))
    got = [halves(rb[:, c * s : (c + 1) * s, :].reshape(lines, width) * 0.015625) for c in (0, 2, 1, 3)]

    def triple(c, b):
        return (b, 2.0 * (c + b), c)

    def nine(v):
        by_x0 = triple(v[0], v[1])
        by_x1 = triple(v[2], v[3])
        return [triple(by_x0[o1], by_x1[o1]) for o1 in range(3)]

    def copies(first, count):
        part = pl.ds(first, count)
        return (
            pltpu.make_async_copy(out_ref.at[:, part, :], out_hbm.at[:, part, :], sem),
            pltpu.make_async_copy(lump_ref.at[part, :], lump_hbm.at[part, :], sem),
        )

    first = 0
    for count, piece in parts:
        to_slot = onehot(slot == iota((count, lines), 0) + first)
        for c in range(4):
            hi, lo = got[c]
            cur[c, first : first + count, :] = lax.dot_general(to_slot, hi, NN, preferred_element_type=F32) + lax.dot_general(
                to_slot, lo, NN, preferred_element_type=F32
            )
        hi, lo = rims
        bef[first : first + count, :] = lax.dot_general(to_slot, hi, NT, preferred_element_type=F32) + lax.dot_general(
            to_slot, lo, NT, preferred_element_type=F32
        )
        for start in range(first, first + count, piece):
            span = slice(start, start + piece)
            at_0 = iota((piece, width), 1) == 0
            near, far = [], []
            for c in range(4):
                x = cur[c, span, :]
                near.append(x)
                far.append(jnp.where(at_0, bef[span, c : c + 1] * 0.015625, pltpu.roll(x, 1, axis=1)))
            ahead, back = nine(near), nine(far)
            for o1 in range(3):
                for o2 in range(3):
                    for o3, value in enumerate(triple(ahead[o1][o2], back[o1][o2])):
                        out_ref[9 * o1 + 3 * o2 + o3, span, :] = value
            total = functools.reduce(lambda a, b: a + b, near + far)
            lump_ref[span, :] = 1.0 / (27.0 * total)
            for copy in copies(start, piece):
                copy.start()
        first += count
    for copy in copies(0, lines):
        copy.wait()


def shards(sizes, cell_volume, exponent, owner_row):
    sx, sy, width = cell_volume.shape
    lines = sx * sy
    n = sizes[0] * sizes[1] * sizes[2]
    s = lines // n
    vmem = pl.BlockSpec(memory_space=pltpu.VMEM)
    dma = pltpu.SemaphoreType.DMA
    received = pl.pallas_call(
        functools.partial(exchange, sizes),
        out_shape=jax.ShapeDtypeStruct((n, 4 * s + 1, width), F32),
        in_specs=[pl.BlockSpec(memory_space=pltpu.HBM)] * 3,
        out_specs=vmem,
        scratch_shapes=[
            pltpu.VMEM((sx, sy, width), F32),
            pltpu.VMEM((sx, sy, width), I32),
            pltpu.VMEM((1, lines), I32),
            dma((2,)),
        ]
        + [
            pltpu.VMEM((n, 4 * s + 1, width), F32),
            pltpu.VMEM((sy, width), F32),
            pltpu.VMEM((sx, 1, width), F32),
            pltpu.VMEM((1, width), F32),
            pltpu.VMEM((1, lines), F32),
            pltpu.VMEM((sy, width), F32),
            pltpu.VMEM((sx, 1, width), F32),
            pltpu.VMEM((1, width), F32),
            pltpu.VMEM((4, 1, lines), F32),
            dma,
            dma,
            dma((2,)),
            dma((3,)),
            pltpu.SemaphoreType.REGULAR,
            pltpu.SemaphoreType.REGULAR,
        ]
        + [
            pltpu.VMEM((n // 2, 4 * s + 1, width), F32),
            pltpu.VMEM((lines, width), F32),
            pltpu.VMEM((lines, width), F32),
            pltpu.VMEM((1, lines), I32),
            pltpu.VMEM((sy, width), F32),
            pltpu.VMEM((sx, 1, width), F32),
            pltpu.VMEM((1, width), F32),
            pltpu.VMEM((4, 1, lines), F32),
            pltpu.VMEM((2 * n * (4 * s + 1), width), F32),
        ],
        compiler_params=pltpu.CompilerParams(
            collective_id=0, has_side_effects=True, vmem_limit_bytes=16 << 20
        ),
    )(*(pltpu.with_memory_space_constraint(a, pltpu.HBM) for a in (cell_volume, exponent, owner_row.reshape(1, lines))))
    parts = [(lines // 4, lines // 8)] * 4
    return pl.pallas_call(
        functools.partial(finish, n, parts),
        out_shape=(
            jax.ShapeDtypeStruct((27, lines, width), F32),
            jax.ShapeDtypeStruct((lines, width), F32),
        ),
        in_specs=[vmem],
        out_specs=(pl.BlockSpec(memory_space=pltpu.HBM), pl.BlockSpec(memory_space=pltpu.HBM)),
        scratch_shapes=[
            pltpu.VMEM((4, lines, width), F32),
            pltpu.VMEM((lines, width), F32),
            pltpu.VMEM((27, lines, width), F32),
            pltpu.VMEM((lines, width), F32),
            dma,
        ],
        compiler_params=pltpu.CompilerParams(vmem_limit_bytes=16 << 20),
    )(received)


def solution(mesh):
    sizes = tuple(mesh.shape[a] for a in AXES)
    return jax.shard_map(
        functools.partial(shards, sizes),
        mesh=mesh,
        in_specs=(P(*AXES), P(*AXES), P(AXES)),
        out_specs=(P(None, AXES, None), P(AXES, None)),
        check_vma=False,
    )
```

```python
import functools

import jax
import jax.numpy as jnp
from jax import lax
from jax.experimental import pallas as pl
from jax.experimental.pallas import tpu as pltpu
from jax.sharding import PartitionSpec as P

MESH = pl.DeviceIdType.MESH
AXES = ("gx", "gy", "gz")
F32, BF16, I32 = jnp.float32, jnp.bfloat16, jnp.int32
log_step = 0.3
NN = (((1,), (0,)), ((), ()))
NT = (((1,), (1,)), ((), ()))


def onehot(mask):
    return jnp.where(mask, 1.0, 0.0).astype(BF16)


def halves(x):
    hi = x.astype(BF16)
    return hi, (x - hi.astype(F32)).astype(BF16)


def pick(sel, x, dims=NN):
    total = None
    for part in halves(x):
        term = lax.dot_general(sel, part, dims, preferred_element_type=F32)
        total = term if total is None else total + term
    return total


def pick_r(x, sel, dims=NN):
    total = None
    for part in halves(x):
        term = lax.dot_general(part, sel, dims, preferred_element_type=F32)
        total = term if total is None else total + term
    return total


def iota(shape, dim):
    return lax.broadcasted_iota(I32, shape, dim)


def roll_lanes(x, shift):
    width = x.shape[1]
    cut = width - shift % width
    return jnp.concatenate([x[:, cut:], x[:, :cut]], axis=1)


def exchange(
    sizes, cv_hbm, ex_hbm, own_hbm, rb,
    cv_ref, ex_ref, own_ref, in_sem,
    sb, tx, ty, tc, tr, hx, hy, hc, hr,
    s_sem, r_sem, h_sem, v_sem, ready, above,
    vb, wv, raw, raw_own, vx, vy, vc, vr, tally,
):
    nx, ny, nz = sizes
    plane = ny * nz
    n = nx * plane
    gx, gy, gz = (lax.axis_index(a) for a in AXES)
    here = gy * nz + gz
    me = gx * plane + here
    sx, sy, width = cv_ref.shape
    lines = sx * sy
    s = lines // n
    relay = nx == 4
    half = n // 2
    base = (gx // 2) * 2
    middle = (gx == 1) | (gx == 2)
    across, beside = (gx + 2) % nx, jnp.where(gx < 2, 1 - gx, nx + 1 - gx)
    give, take = jnp.where(middle, beside, across), jnp.where(middle, across, beside)
    theirs = take * plane + here
    spots = [(y, z) for y in range(ny) for z in range(nz)]
    ux, uy, uz = (gx + 1) % nx, (gy + 1) % ny, (gz + 1) % nz
    dx, dy, dz = (gx + nx - 1) % nx, (gy + ny - 1) % ny, (gz + nz - 1) % nz

    def signal(sem, to):
        pl.semaphore_signal(sem, inc=1, device_id=to, device_id_type=MESH)

    def others(visit):
        for y in range(ny):
            for z in range(nz):
                if y or z:
                    visit((gy + y) % ny, (gz + z) % nz)

    def done(rows, sem):
        part = tally.at[pl.ds(0, rows)]
        pltpu.make_async_copy(part, part, sem).wait()

    edge_rows = sx + sy + 1 + 4 * lines // width
    pair_rows = 4 * s + 1
    down_rows = sx + 2 * lines // width

    scope = jax.named_scope
    with scope("a_in"):
        arrive = []
        for i, (src, dst) in enumerate(((own_hbm, own_ref), (cv_hbm, cv_ref), (ex_hbm, ex_ref))):
            copy = pltpu.make_async_copy(src, dst, in_sem.at[min(i, 1)])
            copy.start()
            arrive.append(copy)
    with scope("b_bar"):
        barrier = pltpu.get_barrier_semaphore()
        others(lambda y, z: signal(barrier, (gx, y, z)))
        corners = [(dy, gz), (gy, dz), (dy, dz)]

        @pl.when(gx > 0)
        def _():
            for y, z in corners:
                signal(barrier, (dx, y, z))

        def greet_below(p, carry):
            signal(barrier, (p, gy, gz))
            return carry

        reach = 1 if relay else nx
        lax.fori_loop(jnp.maximum(gx - reach, 0), gx, greet_below, 0)

        def greet_above(p, carry):
            if relay:

                @pl.when(p == 1)
                def _():
                    for y, z in [(gy, gz), *corners]:
                        signal(barrier, (p, y, z))

                @pl.when(p > 1)
                def _():
                    for y, z in spots:
                        signal(barrier, (p, y, z))
            else:
                for y, z in spots:
                    signal(barrier, (p, y, z))
            return carry

        lax.fori_loop(gx + 1, nx, greet_above, 0)
        expect = plane - 1 + gx * plane + jnp.minimum(nx - 1 - gx, reach) + jnp.where(gx < nx - 1, len(corners), 0)
        if relay:
            expect -= jnp.where(gx == 1, plane - 1 - len(corners), 0)

    with scope("c_own"):
        arrive[0].wait()
        def ranks(own):
            owner = own // lines
            mine = owner == iota((n, lines), 0)
            counts = lax.dot_general(onehot(mine), below, NN, preferred_element_type=F32)
            rank = jnp.sum(jnp.where(mine, counts, 0.0), axis=0, keepdims=True).astype(I32)
            return onehot(mine), rank, owner * s + rank, (own % lines).astype(F32)

        below = onehot(iota((lines, lines), 0) < iota((lines, lines), 1))
        mine_b, rank, goes, slot = ranks(own_ref[...])
        place = onehot(goes == iota((lines, lines), 0))
        row_id = iota((width, lines), 0)
        group = row_id // s

    with scope("d_inwait"):
        done(2 * lines, in_sem.at[1])
    with scope("e_pack0"):
        w3 = cv_ref[...] * jnp.exp(-log_step * ex_ref[...].astype(F32))
        w = w3.reshape(lines, width)
        wv[...] = w
        tx[...] = w[lines - sy :, :]
        ty[...] = w3[:, sy - 1 :, :]
        tc[...] = w[lines - 1 :, :]
        last = onehot(iota((8, width), 1) == width - 1)
        tr[...] = pick(last, w, NT)[0:1, :]
        sb[:, 0:s, :] = pick(place, w).reshape(n, s, width)

    with scope("g_barwait"):
        pl.semaphore_wait(barrier, expect)
        others(lambda y, z: signal(ready, (gx, y, z)))
        if relay:

            @pl.when(gx == 1)
            def _():
                signal(above, (0, gy, gz))


    with scope("h_halosend"):
        routes = [
            (tx, hx, (ux, gy, gz)),
            (ty, hy, (gx, uy, gz)),
            (tc, hc, (ux, uy, gz)),
            (tr, hr.at[0], (gx, gy, uz)),
            (tr, hr.at[1], (ux, gy, uz)),
            (tr, hr.at[2], (gx, uy, uz)),
            (tr, hr.at[3], (ux, uy, uz)),
        ]
        for i, (src, dst, to) in enumerate(routes):
            copy = pltpu.make_async_remote_copy(
                src_ref=src, dst_ref=dst, send_sem=s_sem, recv_sem=h_sem.at[0 if src is ty else 1],
                device_id=to, device_id_type=MESH,
            )
            copy.start()

    def hand(sem, src, dst, to):
        return pltpu.make_async_remote_copy(
            src_ref=src, dst_ref=dst, send_sem=s_sem, recv_sem=sem, device_id=to, device_id_type=MESH
        )

    raw_copies = [hand(v_sem.at[2], own_ref, raw_own, (give, gy, gz)), hand(v_sem.at[1], wv, raw, (give, gy, gz))]
    back = jnp.maximum(gx - 1, 0)
    back_copies = [
        hand(v_sem.at[0], tx, vx, (back, gy, gz)),
        hand(v_sem.at[0], tc, vc, (back, uy, gz)),
        hand(v_sem.at[0], tr, vr.at[1], (back, gy, uz)),
        hand(v_sem.at[0], tr, vr.at[3], (back, uy, uz)),
    ]
    side_copies = [
        hand(v_sem.at[0], ty, vy, (across, uy, gz)),
        hand(v_sem.at[0], tr, vr.at[0], (across, gy, uz)),
        hand(v_sem.at[0], tr, vr.at[2], (across, uy, uz)),
    ]
    edge_copies = [
        hand(v_sem.at[0], src, dst, (give, gy, gz)) for src, dst in ((hx, vx), (hy, vy), (hc, vc), (hr, vr))
    ]

    down_copies = [
        hand(v_sem.at[0], ty, vy, (back, uy, gz)),
        hand(v_sem.at[0], tr, vr.at[0], (back, gy, uz)),
        hand(v_sem.at[0], tr, vr.at[2], (back, uy, uz)),
    ]
    flat_copies = [hand(v_sem.at[0], tc, vc, (gx, uy, gz))]

    def part_to(p, y, z, first, count):
        d, part = p * plane + y * nz + z, pl.ds(first, count)
        pltpu.make_async_remote_copy(
            src_ref=sb.at[d, part], dst_ref=rb.at[me, part], send_sem=s_sem, recv_sem=r_sem,
            device_id=(p, y, z), device_id_type=MESH,
        ).start()

    early = s if relay and s % 8 == 0 else 0

    def start_when(flag, copies):
        @pl.when(flag)
        def _():
            for copy in copies:
                copy.start()

    if relay:
        with scope("h_raw"):
            start_when(gx >= 2, back_copies)
            start_when(gx == 1, down_copies)
            start_when(gx == 0, flat_copies)
            start_when(gx == nx - 1, side_copies)
            start_when(gx > 0, raw_copies)
            if early:

                @pl.when(gx == 2)
                def _():
                    for y, z in spots:
                        part_to(0, y, z, 0, early)


    def send_one(p, y, z):
        pltpu.make_async_remote_copy(
            src_ref=sb.at[p * plane + y * nz + z], dst_ref=rb.at[me], send_sem=s_sem, recv_sem=r_sem,
            device_id=(p, y, z), device_id_type=MESH,
        ).start()

    low, top = 0, nx - 1
    if relay:
        low = jnp.where(gx == 2, 0, jnp.where(gx == 1, 1, base))
        top = jnp.where(gx == 1, nx - 1, jnp.where(gx == 2, 2, base + 1))

    def send_below():
        def send(p, carry):
            for y, z in spots:
                send_one(p, y, z)
            return carry

        if relay:

            @pl.when(gx == 2)
            def _():
                for y, z in spots:
                    part_to(0, y, z, early, pair_rows - early)

        lax.fori_loop(jnp.maximum(low, 1) if relay else 0, gx, send, 0)

    def send_above():
        def send(k, carry):
            for y, z in spots:
                send_one(top - k, y, z)
            return carry

        lax.fori_loop(0, top - gx, send, 0)

    def send_plane(first, count):
        others(lambda y, z: part_to(gx, y, z, first, count))

    split = 2 * s if (2 * s) % 8 == 0 else 0

    with scope("j_ready"):
        pl.semaphore_wait(ready, plane - 1)
    with scope("k_send0"):
        if relay:

            @pl.when(gx == 2)
            def _():
                signal(above, (1, gy, gz))

            @pl.when(gx == 0)
            def _():
                pl.semaphore_wait(above, 1)

            start_when(gx == 0, side_copies + raw_copies)

    line_id = iota((lines, width), 0)
    first_j = line_id % sy == 0
    lane = iota((1, lines), 1)
    at_j0 = lane % sy == 0

    def back_j(x, edge):
        edge_full = jnp.broadcast_to(edge, (sx, sy, width)).reshape(lines, width)
        shifted = jnp.concatenate([x[lines - 1 :, :], x[: lines - 1, :]], axis=0)
        return jnp.where(first_j, edge_full, shifted)

    def behind_i(w, hx, hy, hc):
        x1 = jnp.concatenate([hx[...], w[: lines - sy, :]], axis=0)
        return x1, back_j(x1, jnp.concatenate([hc[...].reshape(1, 1, width), hy[...][: sx - 1]], axis=0))

    def rim_rows(hr, mine_b, rank, slot):
        r0, rx, ry, rxy = hr[0], hr[1], hr[2], hr[3]
        rim1 = jnp.where(lane < sy, roll_lanes(rx, sy), roll_lanes(r0, sy))
        rim2 = jnp.where(at_j0, roll_lanes(ry, 1 - sy), roll_lanes(r0, 1))
        edge_rim = jnp.where(lane == 0, roll_lanes(rxy, 1), roll_lanes(ry, 1))
        rim3 = jnp.where(at_j0, edge_rim, roll_lanes(rim1, 1))
        rims = slot
        for q, rim in enumerate((r0, rim1, rim2, rim3)):
            rims = jnp.where(group == q, rim, rims)
        rims = jnp.where((rank == row_id % s) & (group < 5), rims, 0.0)
        return pick(mine_b, rims, NT)

    with scope("l_halo0"):
        done(sx, h_sem.at[0])
    with scope("l_pack"):
        sb[:, s : 2 * s, :] = pick(place, back_j(w, hy[...])).reshape(n, s, width)
        if split:
            send_plane(0, split)
    with scope("l_halo1"):
        done(edge_rows - sx, h_sem.at[1])
        if relay:
            start_when(gx == 2, edge_copies)
    with scope("m_pack1"):
        for c, x in enumerate(behind_i(w, hx, hy, hc)):
            sb[:, (c + 2) * s : (c + 3) * s, :] = pick(place, x).reshape(n, s, width)
        sb[:, 4 * s : 4 * s + 1, :] = rim_rows(hr, mine_b, rank, slot).reshape(n, 1, width)

    with scope("n_send1"):
        send_below()
        send_plane(split, pair_rows - split)
        pltpu.make_async_copy(sb.at[me], rb.at[me], r_sem).start()
        if relay:

            @pl.when(gx == 1)
            def _():
                pl.semaphore_wait(above, 1)

        send_above()

    def send_theirs():
        end = jnp.where(gx == 1, 0, nx - 1)

        def to(p, y, z):
            pltpu.make_async_remote_copy(
                src_ref=vb.at[(p - base) * plane + y * nz + z], dst_ref=rb.at[theirs], send_sem=s_sem, recv_sem=r_sem,
                device_id=(p, y, z), device_id_type=MESH,
            ).start()

        @pl.when(middle)
        def _():
            for y, z in spots:
                to(end, y, z)

        others(lambda y, z: to(gx, y, z))
        pltpu.make_async_copy(vb.at[(gx - base) * plane + here], rb.at[theirs], r_sem).start()

    if relay:
        with scope("o_prep"):
            done(lines // width, v_sem.at[2])
            _, rank_v, goes_v, slot_v = ranks(raw_own[...])
            place_v = onehot(goes_v - base * plane * s == iota((lines // 2, lines), 0))
            mine_v = onehot(raw_own[...] // lines - base * plane == iota((half, lines), 0))
        with scope("o_wait0"):
            @pl.when(gx == 0)
            def _():
                done(down_rows + 1, v_sem.at[0])
                vx[...] = tx[...]
                vr[1] = hr[0]
                vr[3] = hr[2]

            @pl.when(gx > 0)
            def _():
                done(edge_rows, v_sem.at[0])

        with scope("o_rim"):
            vb[:, 4 * s : 4 * s + 1, :] = rim_rows(vr, mine_v, rank_v, slot_v).reshape(half, 1, width)
        with scope("o_wait1"):
            done(lines, v_sem.at[1])
        with scope("o_pack"):
            x0 = raw[...]
            for c, x in enumerate((x0, back_j(x0, vy[...]), *behind_i(x0, vx, vy, vc))):
                vb[:, c * s : (c + 1) * s, :] = pick(place_v, x).reshape(half, s, width)
        with scope("o_send"):
            send_theirs()

    with scope("q_wait"):
        done(n * pair_rows, r_sem)
    with scope("w_drain"):
        if relay:
            count = edge_rows + lines + lines // width
            back_rows = sy + 1 + 2 * lines // width

            @pl.when(gx >= 2)
            def _():
                done(back_rows, s_sem)


            @pl.when(middle)
            def _():
                done(count + down_rows + (n - plane - 1 + half - 1) * pair_rows, s_sem)

            @pl.when(gx == 2)
            def _():
                done(edge_rows - down_rows, s_sem)

            @pl.when(gx == 0)
            def _():
                done(1, s_sem)

            @pl.when(jnp.logical_not(middle))
            def _():
                done(count + down_rows + (half - 1 + plane - 1) * pair_rows, s_sem)

        else:
            done(edge_rows + (n - 1) * pair_rows, s_sem)


def finish(n, parts, rb, out_hbm, lump_hbm, cur, bef, out_ref, lump_ref, sem):
    lines, width = lump_ref.shape
    s = lines // n
    extra = rb[:, 4 * s : 4 * s + 1, :]
    spread = jnp.broadcast_to(extra, (n, s, width)).reshape(lines, width)
    spread = jnp.where(iota((lines, width), 1) % s == iota((lines, width), 0) % s, spread, 0.0)
    sums = onehot(iota((8, width), 1) // s == iota((8, width), 0))
    rows = pick(sums, spread, NT)
    slot = rows[4:5, :].astype(I32)
    rims = halves(jnp.concatenate([rows, jnp.zeros((width - 8, lines), F32)], axis=0))
    got = [halves(rb[:, c * s : (c + 1) * s, :].reshape(lines, width) * 0.015625) for c in (0, 2, 1, 3)]

    def triple(c, b):
        return (b, 2.0 * (c + b), c)

    def nine(v):
        by_x0 = triple(v[0], v[1])
        by_x1 = triple(v[2], v[3])
        return [triple(by_x0[o1], by_x1[o1]) for o1 in range(3)]

    def copies(first, count):
        part = pl.ds(first, count)
        return (
            pltpu.make_async_copy(out_ref.at[:, part, :], out_hbm.at[:, part, :], sem),
            pltpu.make_async_copy(lump_ref.at[part, :], lump_hbm.at[part, :], sem),
        )

    first = 0
    for count, piece in parts:
        to_slot = onehot(slot == iota((count, lines), 0) + first)
        for c in range(4):
            hi, lo = got[c]
            cur[c, first : first + count, :] = lax.dot_general(to_slot, hi, NN, preferred_element_type=F32) + lax.dot_general(
                to_slot, lo, NN, preferred_element_type=F32
            )
        hi, lo = rims
        bef[first : first + count, :] = lax.dot_general(to_slot, hi, NT, preferred_element_type=F32) + lax.dot_general(
            to_slot, lo, NT, preferred_element_type=F32
        )
        for start in range(first, first + count, piece):
            span = slice(start, start + piece)
            at_0 = iota((piece, width), 1) == 0
            near, far = [], []
            for c in range(4):
                x = cur[c, span, :]
                near.append(x)
                far.append(jnp.where(at_0, bef[span, c : c + 1] * 0.015625, pltpu.roll(x, 1, axis=1)))
            ahead, back = nine(near), nine(far)
            for o1 in range(3):
                for o2 in range(3):
                    for o3, value in enumerate(triple(ahead[o1][o2], back[o1][o2])):
                        out_ref[9 * o1 + 3 * o2 + o3, span, :] = value
            total = functools.reduce(lambda a, b: a + b, near + far)
            lump_ref[span, :] = 1.0 / (27.0 * total)
            for copy in copies(start, piece):
                copy.start()
        first += count
    for copy in copies(0, lines):
        copy.wait()


def shards(sizes, cell_volume, exponent, owner_row):
    sx, sy, width = cell_volume.shape
    lines = sx * sy
    n = sizes[0] * sizes[1] * sizes[2]
    s = lines // n
    vmem = pl.BlockSpec(memory_space=pltpu.VMEM)
    dma = pltpu.SemaphoreType.DMA
    received = pl.pallas_call(
        functools.partial(exchange, sizes),
        out_shape=jax.ShapeDtypeStruct((n, 4 * s + 1, width), F32),
        in_specs=[pl.BlockSpec(memory_space=pltpu.HBM)] * 3,
        out_specs=vmem,
        scratch_shapes=[
            pltpu.VMEM((sx, sy, width), F32),
            pltpu.VMEM((sx, sy, width), I32),
            pltpu.VMEM((1, lines), I32),
            dma((2,)),
        ]
        + [
            pltpu.VMEM((n, 4 * s + 1, width), F32),
            pltpu.VMEM((sy, width), F32),
            pltpu.VMEM((sx, 1, width), F32),
            pltpu.VMEM((1, width), F32),
            pltpu.VMEM((1, lines), F32),
            pltpu.VMEM((sy, width), F32),
            pltpu.VMEM((sx, 1, width), F32),
            pltpu.VMEM((1, width), F32),
            pltpu.VMEM((4, 1, lines), F32),
            dma,
            dma,
            dma((2,)),
            dma((3,)),
            pltpu.SemaphoreType.REGULAR,
            pltpu.SemaphoreType.REGULAR,
        ]
        + [
            pltpu.VMEM((n // 2, 4 * s + 1, width), F32),
            pltpu.VMEM((lines, width), F32),
            pltpu.VMEM((lines, width), F32),
            pltpu.VMEM((1, lines), I32),
            pltpu.VMEM((sy, width), F32),
            pltpu.VMEM((sx, 1, width), F32),
            pltpu.VMEM((1, width), F32),
            pltpu.VMEM((4, 1, lines), F32),
            pltpu.VMEM((2 * n * (4 * s + 1), width), F32),
        ],
        compiler_params=pltpu.CompilerParams(
            collective_id=0, has_side_effects=True, vmem_limit_bytes=16 << 20
        ),
    )(*(pltpu.with_memory_space_constraint(a, pltpu.HBM) for a in (cell_volume, exponent, owner_row.reshape(1, lines))))
    parts = [(lines // 4, lines // 8)] * 4
    return pl.pallas_call(
        functools.partial(finish, n, parts),
        out_shape=(
            jax.ShapeDtypeStruct((27, lines, width), F32),
            jax.ShapeDtypeStruct((lines, width), F32),
        ),
        in_specs=[vmem],
        out_specs=(pl.BlockSpec(memory_space=pltpu.HBM), pl.BlockSpec(memory_space=pltpu.HBM)),
        scratch_shapes=[
            pltpu.VMEM((4, lines, width), F32),
            pltpu.VMEM((lines, width), F32),
            pltpu.VMEM((27, lines, width), F32),
            pltpu.VMEM((lines, width), F32),
            dma,
        ],
        compiler_params=pltpu.CompilerParams(vmem_limit_bytes=16 << 20),
    )(received)


def solution(mesh):
    sizes = tuple(mesh.shape[a] for a in AXES)
    return jax.shard_map(
        functools.partial(shards, sizes),
        mesh=mesh,
        in_specs=(P(*AXES), P(*AXES), P(AXES)),
        out_specs=(P(None, AXES, None), P(AXES, None)),
        check_vma=False,
    )
```
